32 devices in a mesh: shard: 8 (over y, x, core), model: 4 (over z).
Axes of the slice: x: 2, y: 2, z: 4, core: 2. Of those that a mesh axis runs over, the one named last changes fastest.
Arguments:
- weight_gate: float32 [3072, 8192], P('shard', 'model'), may hold values from -0.15625 to 0.15625
- smooth_gate: float32 [3072, 8192], P('shard', 'model'), may hold values from -0.109375 to 0.109375
- weight_up: float32 [3072, 8192], P('shard', 'model'), may hold values from -0.15625 to 0.15625
- smooth_up: float32 [3072, 8192], P('shard', 'model'), may hold values from -0.109375 to 0.109375
- norm_train: float32 [3072], P(('shard', 'model')), may hold values from 0.25 to 1.75
- norm_step: float32 [3072], P(('shard', 'model')), may hold values from -0.3 to 0.3
Outputs:
- serving_gate: bfloat16 [3072, 8192], P(None, 'model')
- serving_up: bfloat16 [3072, 8192], P(None, 'model')
- factor_gate: float32 [8192], P('model')
- factor_up: float32 [8192], P('model')
- serve_norm: bfloat16 [3072], replicated
- whole_gate: float32 [3072, 8192], P('shard', 'model')
- whole_up: float32 [3072, 8192], P('shard', 'model')
The draws below stay inside these ranges and needn't reach their ends.
All inputs are finite; a program needn't handle non-finite values. Where the reference program divides by a largest or mean magnitude, that divisor is 1e-20 or more.
Results may differ from the reference program's by a relative error of at most 0.001.
Values may be sent and summed in bfloat16 or wider, within the bound.
A program may use at most 128 MiB of HBM per device.

```python
import jax
import jax.numpy as jnp

D_MODEL = 3072
D_INNER = 8192


def raised(result, key, source, target, blocks, factor):
    owner, partner = [(jnp.arange(result.shape[dim]) // (result.shape[dim] // blocks)).reshape([-1 if axis == dim else 1 for axis in range(result.ndim)]) for dim in (source, target)]
    chosen = jax.random.permutation(key, blocks)[partner]
    strong = (owner == chosen) | (owner == (partner + blocks // 2) % blocks)
    return jnp.where(strong, factor * result, result)


def block_levels(rng, extent, split, smallest, top_value):
    def one(dim, blocks):
        heights = jax.random.uniform(jax.random.fold_in(jax.random.fold_in(rng, 6), dim), (blocks,), jnp.float32, smallest / len(split), top_value / len(split))
        return jnp.repeat(jnp.exp(heights), extent[dim] // blocks).reshape((-1,) + (1,) * (len(extent) - dim - 1))

    level = one(*split[0])
    for cut in split[1:]:
        level = level * one(*cut)
    return level


def scatter_about(stream_key, dims, scale, most, pieces=(), kind=jnp.bfloat16):
    factor_of = block_levels(stream_key, dims, pieces, -0.22, 0.18) if pieces else 1.0
    values = jax.random.normal(stream_key, dims, jnp.float32) * scale * factor_of
    return jnp.minimum(jnp.maximum(values, -most), most).astype(kind)


def noise_with(key, dims, scale, limit, cuts, heavy, kind=jnp.bfloat16):
    values = scale * jax.random.normal(key, dims, jnp.float32)
    if cuts:
        values = values * block_levels(key, dims, cuts, -0.22, 0.18)
    return jnp.clip(raised(values, jax.random.fold_in(key, 3), *heavy), -limit, limit).astype(kind)


def setup_inputs(seed: int = 0) -> dict:
    arg_keys = jax.random.split(jax.random.key(seed), 7)
    return {
        "weight_gate": noise_with(arg_keys[0], (D_MODEL, D_INNER), D_MODEL ** -0.5, 0.15625, ((0, 8), (1, 4)), (0, 1, 8, 2.0), jnp.float32),
        "smooth_gate": scatter_about(arg_keys[1], (D_MODEL, D_INNER), D_MODEL ** -0.5, 0.109375, ((0, 8), (1, 4)), jnp.float32),
        "weight_up": noise_with(arg_keys[2], (D_MODEL, D_INNER), D_MODEL ** -0.5, 0.15625, ((0, 8), (1, 4)), (0, 1, 8, 2.0), jnp.float32),
        "smooth_up": scatter_about(arg_keys[3], (D_MODEL, D_INNER), D_MODEL ** -0.5, 0.109375, ((0, 8), (1, 4)), jnp.float32),
        "norm_train": jnp.clip(1.0 + 0.15 * jax.random.normal(arg_keys[4], (D_MODEL,), jnp.float32), 0.25, 1.75),
        "norm_step": jnp.clip(jax.random.uniform(arg_keys[5], (D_MODEL,), jnp.float32, -0.3, 0.3) * block_levels(arg_keys[5], (D_MODEL,), ((0, 32),), -0.4, 0.0), -0.3, 0.3),
    }


keep_rate = 0.7


def reference(weight_gate, smooth_gate, weight_up, smooth_up, norm_train, norm_step):
    whole_gate = keep_rate * smooth_gate + (1.0 - keep_rate) * weight_gate
    whole_up = keep_rate * smooth_up + (1.0 - keep_rate) * weight_up
    factor_gate = jnp.max(jnp.abs(whole_gate), axis=0)
    serving_gate = (whole_gate / factor_gate).astype(jnp.bfloat16)
    factor_up = jnp.max(jnp.abs(whole_up), axis=0)
    serving_up = (whole_up / factor_up).astype(jnp.bfloat16)
    serve_norm = (norm_train + norm_step).astype(jnp.bfloat16)
    return serving_gate, serving_up, factor_gate, factor_up, serve_norm, whole_gate, whole_up
```

```python
import functools
import math

import jax
import jax.numpy as jnp
from jax import lax
from jax.experimental import pallas as pl
from jax.experimental.pallas import tpu as pltpu
from jax.sharding import PartitionSpec as P

MESH = pl.DeviceIdType.MESH
keep_rate = 0.7
LANES = 128


def grid_of(n_shard):
    chips = n_shard // 2
    nx = math.isqrt(chips)
    while chips % nx:
        nx -= 1
    return chips // nx, nx


def widths_of(tiles, unit):
    if tiles < 4:
        return [1] * tiles
    if unit == 0:
        return [1, 2, tiles - 3]
    return [tiles // 2, tiles - tiles // 2 - 1, 1]


def pieces_of(cols):
    tiles = cols // LANES
    found = []
    for unit in range(2):
        queues = [(True, widths_of((tiles + 1) // 2, unit)), (False, widths_of(tiles // 2, unit))]
        at = 0
        for n in range(max(len(q) for _, q in queues)):
            for along_x, queue in queues:
                if n < len(queue):
                    found.append((unit, at * LANES, queue[n] * LANES, along_x, unit == 0 and n == 0))
                    at += queue[n]
    return found


def kernel(
    n_shard, n_model, ny, nx, pieces,
    weight_gate, smooth_gate, weight_up, smooth_up, norm_train, norm_step,
    serve_gate, serve_up, factor_gate, factor_up, norm_out, whole_gate, whole_up,
    weights, smooths, peaks, early, norm_in, norm_all, norm_rows,
    load_sem, norm_load, peak_send, peak_recv, norm_send, norm_recv, row_send, row_recv,
    x_send, y_send, pair_send, ring_recv, pair_recv,
):
    me = lax.axis_index("shard")
    col = lax.axis_index("model")
    core = lax.rem(me, 2)
    chip = me // 2
    xpos, ypos = lax.rem(chip, nx), chip // nx
    x_next = (ypos * nx + lax.rem(xpos + 1, nx)) * 2 + core
    y_next = (lax.rem(ypos + 1, ny) * nx + xpos) * 2 + core
    pair = chip * 2 + (1 - core)
    rows, cols = whole_gate.shape
    serves, wholes, factors = (serve_gate, serve_up), (whole_gate, whole_up), (factor_gate, factor_up)
    count = len(pieces)
    order = range(count)
    early_pieces = [p for p in order if pieces[p][4]]
    first = len(early_pieces)

    def across(p):
        return pl.ds(pieces[p][1], pieces[p][2])

    sources = ((weight_gate, smooth_gate), (weight_up, smooth_up))
    loads = {}
    for p in order:
        unit = pieces[p][0]
        for which, dst in enumerate((weights, smooths)):
            copy = pltpu.make_async_copy(
                sources[unit][which].at[:, across(p)], dst.at[unit, :, across(p)], load_sem.at[p, which]
            )
            copy.start()
            loads[p, which] = copy
        if p == first:
            norm_loads = [
                pltpu.make_async_copy(src, norm_in.at[i], norm_load.at[i])
                for i, src in enumerate((norm_train, norm_step))
            ]
            for copy in norm_loads:
                copy.start()

    barrier = pltpu.get_barrier_semaphore()
    for d in range(1, n_shard):
        pl.semaphore_signal(barrier, inc=1, device_id=(lax.rem(me + d, n_shard), col), device_id_type=MESH)
    for d in range(1, n_model):
        pl.semaphore_signal(barrier, inc=1, device_id=(me, lax.rem(col + d, n_model)), device_id_type=MESH)

    def average(p):
        unit, _, width = pieces[p][:3]
        for which in range(2):
            loads[p, which].wait()

        def step(i, top):
            span = pl.ds(pl.multiple_of(i * 8, 8), 8)
            value = keep_rate * smooths[unit, span, across(p)] + (1.0 - keep_rate) * weights[unit, span, across(p)]
            wholes[unit][span, across(p)] = value
            return jnp.maximum(top, jnp.abs(value))

        top = lax.fori_loop(0, rows // 8, step, jnp.zeros((8, width), jnp.float32), unroll=4)
        peaks[unit, me, :, across(p)] = jnp.max(top, axis=0, keepdims=True)

    peak_copies = {}

    def send_peaks(p):
        unit = pieces[p][0]
        peak_copies[p] = []
        for d in range(1, n_shard):
            ref = peaks.at[unit, me, :, across(p)]
            copy = pltpu.make_async_remote_copy(
                src_ref=ref, dst_ref=ref,
                send_sem=peak_send.at[p, d - 1], recv_sem=peak_recv.at[p, d - 1],
                device_id=(lax.rem(me + d, n_shard), col), device_id_type=MESH,
            )
            copy.start()
            peak_copies[p].append(copy)

    def piece_of(p, dy, dx, side):
        owner = (lax.rem(ypos - dy + ny, ny) * nx + lax.rem(xpos - dx + nx, nx)) * 2 + side
        return serves[pieces[p][0]].at[pl.ds(pl.multiple_of(owner * rows, rows), rows), across(p)]

    sent = []

    def start(src, dst, device, send_sem, recv_sem):
        copy = pltpu.make_async_remote_copy(
            src_ref=src, dst_ref=dst, send_sem=send_sem, recv_sem=recv_sem,
            device_id=(device, col), device_id_type=MESH,
        )
        copy.start()
        sent.append(copy)

    def along_x_first(p):
        return pieces[p][3]

    def to_x(p, dy, dx):
        if dx < nx - 1 and (dy == 0 or not along_x_first(p)):
            ref = piece_of(p, dy, dx, core)
            start(ref, ref, x_next, x_send.at[dy, dx, p], ring_recv.at[dy, dx + 1, p])

    def to_y(p, dy, dx):
        if dy < ny - 1 and (dx == 0 or along_x_first(p)):
            ref = piece_of(p, dy, dx, core)
            start(ref, ref, y_next, y_send.at[dy, dx, p], ring_recv.at[dy + 1, dx, p])

    def to_pair(p, dy, dx):
        ref = piece_of(p, dy, dx, core)
        start(ref, ref, pair, pair_send.at[dy, dx, p], pair_recv.at[dy, dx, p])

    def first_way(p):
        (to_x if along_x_first(p) else to_y)(p, 0, 0)

    def second_way(p):
        (to_y if along_x_first(p) else to_x)(p, 0, 0)

    def send_early(p):
        src = wholes[pieces[p][0]].at[:, across(p)]
        if along_x_first(p):
            if nx > 1:
                start(src, early.at[p], x_next, x_send.at[0, 0, p], ring_recv.at[0, 1, p])
        elif ny > 1:
            start(src, early.at[p], y_next, y_send.at[0, 0, p], ring_recv.at[1, 0, p])

    def landed_early(p, dy, dx):
        return pieces[p][4] and (dy, dx) == ((0, 1) if along_x_first(p) else (1, 0))

    def find_factor(p):
        unit = pieces[p][0]
        for copy in peak_copies[p]:
            copy.wait_recv()
        factor = peaks[unit, 0, :, across(p)]
        for d in range(1, n_shard):
            factor = jnp.maximum(factor, peaks[unit, d, :, across(p)])
        factors[unit][:, across(p)] = factor

    def narrow(p, owner, read):
        unit = pieces[p][0]

        def step(i, carry):
            at = i * 16
            value = read(pl.ds(pl.multiple_of(at, 16), 16)) / factors[unit][:, across(p)]
            serves[unit][pl.ds(pl.multiple_of(owner * rows + at, 16), 16), across(p)] = value.astype(jnp.bfloat16)
            return carry

        lax.fori_loop(0, rows // 16, step, 0, unroll=2)

    def narrow_own(p):
        narrow(p, me, lambda span: wholes[pieces[p][0]][span, across(p)])

    def arrived(p, dy, dx):
        if landed_early(p, dy, dx):
            ref = early.at[p]
            pltpu.make_async_copy(ref, ref, ring_recv.at[dy, dx, p]).wait()
            owner = (lax.rem(ypos - dy + ny, ny) * nx + lax.rem(xpos - dx + nx, nx)) * 2 + core
            narrow(p, owner, lambda span: early[p, span])
        else:
            ref = piece_of(p, dy, dx, core)
            pltpu.make_async_copy(ref, ref, ring_recv.at[dy, dx, p]).wait()

    per = norm_train.shape[1]
    lead = min(first + 2, count)
    for p in range(lead):
        average(p)
    pl.semaphore_wait(barrier, n_shard + n_model - 2)
    for p in range(lead):
        send_peaks(p)
    for p in early_pieces:
        send_early(p)
    for copy in norm_loads:
        copy.wait()
    norm_all[me, col, :, 0:per] = norm_in[0] + norm_in[1]
    for p in range(lead, count):
        average(p)
        if p > lead:
            send_peaks(p - 1)
    if count > lead:
        send_peaks(count - 1)
    norm_copies = []
    for d in range(1, n_model):
        copy = pltpu.make_async_remote_copy(
            src_ref=norm_all.at[me, col], dst_ref=norm_all.at[me, col],
            send_sem=norm_send.at[d - 1], recv_sem=norm_recv.at[d - 1],
            device_id=(me, lax.rem(col + d, n_model)), device_id_type=MESH,
        )
        copy.start()
        norm_copies.append(copy)

    row_copies = []

    def send_rows():
        for copy in norm_copies:
            copy.wait_recv()
        for d in range(1, n_shard):
            copy = pltpu.make_async_remote_copy(
                src_ref=norm_all.at[me], dst_ref=norm_all.at[me],
                send_sem=row_send.at[d - 1], recv_sem=row_recv.at[d - 1],
                device_id=(lax.rem(me + d, n_shard), col), device_id_type=MESH,
            )
            copy.start()
            row_copies.append(copy)

    before = None
    for p in range(first, count):
        find_factor(p)
        if before is not None:
            first_way(before)
        narrow_own(p)
        before = p
    for p in early_pieces:
        find_factor(p)
    if before is not None:
        first_way(before)
    send_rows()
    for p in early_pieces:
        narrow_own(p)
    for p in range(first, count):
        second_way(p)
    for p in early_pieces:
        second_way(p)
    for p in order:
        to_pair(p, 0, 0)

    def gather_norm():
        for copy in row_copies:
            copy.wait_recv()
        lane = lax.broadcasted_iota(jnp.int32, (8, LANES), 1)
        tiles = [jnp.zeros((8, LANES), jnp.float32) for _ in range(norm_out.shape[0])]
        for s in range(n_shard):
            for c in range(n_model):
                for at in range(0, per, LANES):
                    size = min(LANES, per - at)
                    tile, shift = divmod((s * n_model + c) * per + at, LANES)
                    row = jnp.broadcast_to(norm_all[s, c, :, at:at + LANES], (8, LANES))
                    if shift:
                        row = pltpu.roll(row, shift, 1)
                    tiles[tile] = jnp.where((lane >= shift) & (lane < shift + size), row, tiles[tile])
                    if shift + size > LANES:
                        tiles[tile + 1] = jnp.where(lane < shift + size - LANES, row, tiles[tile + 1])
        for t, tile in enumerate(tiles):
            norm_rows[t:t + 1] = tile[0:1]
        norm_out[...] = norm_rows[...].astype(jnp.bfloat16)

    for distance in range(1, ny + nx - 1):
        for own_way in (True, False):
            for p in order:
                for dy in range(ny):
                    dx = distance - dy
                    straight = (dy if along_x_first(p) else dx) == 0
                    if 0 <= dx < nx and straight == own_way:
                        arrived(p, dy, dx)
                        to_x(p, dy, dx)
                        to_y(p, dy, dx)
                        to_pair(p, dy, dx)
            if distance == 1 and own_way:
                gather_norm()

    for p in order:
        for dy in range(ny):
            for dx in range(nx):
                ref = piece_of(p, dy, dx, 1 - core)
                pltpu.make_async_copy(ref, ref, pair_recv.at[dy, dx, p]).wait()
    for copy in sent + sum(peak_copies.values(), []) + norm_copies + row_copies:
        copy.wait_send()


def store_kernel(count, parts, *refs):
    copies = []
    for src, dst in zip(refs[:count], refs[count:-1]):
        pieces = parts if src.shape[0] % (parts * 16) == 0 else 1
        size = src.shape[0] // pieces
        for n in range(pieces):
            span = pl.ds(n * size, size)
            copies.append(pltpu.make_async_copy(src.at[span], dst.at[span], refs[-1].at[len(copies)]))
            copies[-1].start()
    for copy in copies:
        copy.wait()


def store(arrays, parts):
    hbm = pl.BlockSpec(memory_space=pltpu.HBM)
    return pl.pallas_call(
        functools.partial(store_kernel, len(arrays), parts),
        out_shape=tuple(pltpu.HBM(a.shape, a.dtype) for a in arrays),
        in_specs=[pl.BlockSpec(memory_space=pltpu.VMEM)] * len(arrays),
        out_specs=(hbm,) * len(arrays),
        scratch_shapes=[pltpu.SemaphoreType.DMA((len(arrays) * parts,))],
        compiler_params=pltpu.CompilerParams(vmem_limit_bytes=1024 * 1024),
    )(*(pltpu.with_memory_space_constraint(a, pltpu.VMEM) for a in arrays))


def solution(mesh):
    n_shard, n_model = mesh.shape["shard"], mesh.shape["model"]
    ny, nx = grid_of(n_shard)

    def body(weight_gate, smooth_gate, weight_up, smooth_up, norm_train, norm_step):
        rows, cols = weight_gate.shape
        per = norm_train.shape[0]
        pieces = pieces_of(cols)
        count = len(pieces)
        wide = -(-per // LANES) * LANES
        width = n_shard * n_model * per
        tiles = -(-width // LANES)
        vmem = pl.BlockSpec(memory_space=pltpu.VMEM)
        hbm = pl.BlockSpec(memory_space=pltpu.HBM)
        dma = pltpu.SemaphoreType.DMA
        landed = pl.pallas_call(
            functools.partial(kernel, n_shard, n_model, ny, nx, pieces),
            out_shape=(
                pltpu.VMEM((n_shard * rows, cols), jnp.bfloat16),
                pltpu.VMEM((n_shard * rows, cols), jnp.bfloat16),
                pltpu.VMEM((1, cols), jnp.float32),
                pltpu.VMEM((1, cols), jnp.float32),
                pltpu.VMEM((tiles, LANES), jnp.bfloat16),
                pltpu.VMEM((rows, cols), jnp.float32),
                pltpu.VMEM((rows, cols), jnp.float32),
            ),
            in_specs=[hbm] * 6,
            out_specs=(vmem,) * 7,
            scratch_shapes=[
                pltpu.VMEM((2, rows, cols), jnp.float32),
                pltpu.VMEM((2, rows, cols), jnp.float32),
                pltpu.VMEM((2, n_shard, 1, cols), jnp.float32),
                pltpu.VMEM((2, rows, LANES), jnp.float32),
                pltpu.VMEM((2, 1, per), jnp.float32),
                pltpu.VMEM((n_shard, n_model, 1, wide), jnp.float32),
                pltpu.VMEM((tiles, LANES), jnp.float32),
                dma((count, 2)),
                dma((2,)),
                dma((count, n_shard)),
                dma((count, n_shard)),
                dma((n_model,)),
                dma((n_model,)),
                dma((n_shard,)),
                dma((n_shard,)),
                dma((ny, nx, count)),
                dma((ny, nx, count)),
                dma((ny, nx, count)),
                dma((ny, nx, count)),
                dma((ny, nx, count)),
            ],
            compiler_params=pltpu.CompilerParams(
                collective_id=0, has_side_effects=True, vmem_limit_bytes=20 * 1024 * 1024
            ),
        )(
            *(
                pltpu.with_memory_space_constraint(a, pltpu.HBM)
                for a in (weight_gate, smooth_gate, weight_up, smooth_up, norm_train[None], norm_step[None])
            ),
        )
        serve_gate, serve_up, factor_gate, factor_up, norm, whole_gate, whole_up = store(landed, 4)
        return (
            serve_gate, serve_up, factor_gate.reshape(-1), factor_up.reshape(-1),
            norm.reshape(-1)[:width], whole_gate, whole_up,
        )

    in_specs = (P("shard", "model"),) * 4 + (P(("shard", "model")),) * 2
    out_specs = (
        P(None, "model"),
        P(None, "model"),
        P("model"),
        P("model"),
        P(),
        P("shard", "model"),
        P("shard", "model"),
    )
    return jax.shard_map(body, mesh=mesh, in_specs=in_specs, out_specs=out_specs, check_vma=False)
```

```python
import functools
import math

import jax
import jax.numpy as jnp
from jax import lax
from jax.experimental import pallas as pl
from jax.experimental.pallas import tpu as pltpu
from jax.sharding import PartitionSpec as P

MESH = pl.DeviceIdType.MESH
keep_rate = 0.7
LANES = 128


def grid_of(n_shard):
    chips = n_shard // 2
    nx = math.isqrt(chips)
    while chips % nx:
        nx -= 1
    return chips // nx, nx


def widths_of(tiles, unit):
    if tiles < 4:
        return [1] * tiles
    if unit == 0:
        return [1, 2, tiles - 3]
    return [tiles // 2, tiles - tiles // 2 - 1, 1]


def pieces_of(cols, early):
    tiles = cols // LANES
    found = []
    for unit in range(2):
        queues = [(True, widths_of((tiles + 1) // 2, unit)), (False, widths_of(tiles // 2, unit))]
        at = 0
        for n in range(max(len(q) for _, q in queues)):
            for along_x, queue in queues:
                if n < len(queue):
                    found.append((unit, at * LANES, queue[n] * LANES, along_x, early and unit == 0 and n == 0))
                    at += queue[n]
    return found


def kernel(
    n_shard, n_model, ny, nx, pieces,
    weight_gate, smooth_gate, weight_up, smooth_up, norm_train, norm_step,
    serve_gate, serve_up, factor_gate, factor_up, norm_out, whole_gate, whole_up,
    inputs, peaks, early, norm_in, norm_all, norm_rows,
    load_sem, peak_recv, ring_recv, pair_recv, sent_sem, small_sem,
):
    me = lax.axis_index("shard")
    col = lax.axis_index("model")
    core = lax.rem(me, 2)
    chip = me // 2
    xpos, ypos = lax.rem(chip, nx), chip // nx
    x_next = (ypos * nx + lax.rem(xpos + 1, nx)) * 2 + core
    y_next = (lax.rem(ypos + 1, ny) * nx + xpos) * 2 + core
    pair = chip * 2 + (1 - core)
    rows, cols = whole_gate.shape
    serves, wholes, factors = (serve_gate, serve_up), (whole_gate, whole_up), (factor_gate, factor_up)
    count = len(pieces)
    order = range(count)
    early_pieces = [p for p in order if pieces[p][4]]
    first = len(early_pieces)

    def across(p):
        return pl.ds(pieces[p][1], pieces[p][2])

    sources = ((weight_gate, smooth_gate), (weight_up, smooth_up))
    norm_load, norm_send, norm_recv, row_send, row_recv, peak_send = [small_sem.at[i] for i in range(6)]

    def wait_bytes(ref, sem):
        pltpu.make_async_copy(ref, ref, sem).wait()

    for p in order:
        unit = pieces[p][0]
        for which in range(2):
            pltpu.make_async_copy(
                sources[unit][which].at[:, across(p)], inputs.at[which, unit, :, across(p)], load_sem.at[p]
            ).start()
        if p == first:
            for i, src in enumerate((norm_train, norm_step)):
                pltpu.make_async_copy(src, norm_in.at[i], norm_load).start()

    barrier = pltpu.get_barrier_semaphore()
    for d in range(1, n_shard):
        pl.semaphore_signal(barrier, inc=1, device_id=(lax.rem(me + d, n_shard), col), device_id_type=MESH)
    for d in range(1, n_model):
        pl.semaphore_signal(barrier, inc=1, device_id=(me, lax.rem(col + d, n_model)), device_id_type=MESH)

    def average(p):
        unit, _, width = pieces[p][:3]
        wait_bytes(inputs.at[:, unit, :, across(p)], load_sem.at[p])

        def step(i, top):
            span = pl.ds(pl.multiple_of(i * 8, 8), 8)
            value = keep_rate * inputs[1, unit, span, across(p)] + (1.0 - keep_rate) * inputs[0, unit, span, across(p)]
            wholes[unit][span, across(p)] = value
            return jnp.maximum(top, jnp.abs(value))

        top = lax.fori_loop(0, rows // 8, step, jnp.zeros((8, width), jnp.float32), unroll=4)
        peaks[unit, me, :, across(p)] = jnp.max(top, axis=0, keepdims=True)

    def start(src, dst, device, send_sem, recv_sem):
        pltpu.make_async_remote_copy(
            src_ref=src, dst_ref=dst, send_sem=send_sem, recv_sem=recv_sem,
            device_id=device, device_id_type=MESH,
        ).start()

    def send_peaks(p):
        ref = peaks.at[pieces[p][0], me, :, across(p)]
        for d in range(1, n_shard):
            start(ref, ref, (lax.rem(me + d, n_shard), col), peak_send, peak_recv.at[p])

    def piece_of(p, dy, dx, side):
        owner = (lax.rem(ypos - dy + ny, ny) * nx + lax.rem(xpos - dx + nx, nx)) * 2 + side
        return serves[pieces[p][0]].at[pl.ds(pl.multiple_of(owner * rows, rows), rows), across(p)]

    def group_of(p):
        return 2 if pieces[p][4] else pieces[p][0]

    spots = [(dy, dx) for dy in range(ny) for dx in range(nx)][1:]

    def landing(p, dy, dx):
        return ring_recv.at[p * len(spots) + spots.index((dy, dx))]

    def along_x_first(p):
        return pieces[p][3]

    def to_x(p, dy, dx):
        if dx < nx - 1 and (dy == 0 or not along_x_first(p)):
            ref = piece_of(p, dy, dx, core)
            start(ref, ref, (x_next, col), sent_sem.at[group_of(p)], landing(p, dy, dx + 1))

    def to_y(p, dy, dx):
        if dy < ny - 1 and (dx == 0 or along_x_first(p)):
            ref = piece_of(p, dy, dx, core)
            start(ref, ref, (y_next, col), sent_sem.at[group_of(p)], landing(p, dy + 1, dx))

    def to_pair(p, dy, dx):
        ref = piece_of(p, dy, dx, core)
        start(ref, ref, (pair, col), sent_sem.at[group_of(p)], pair_recv.at[pieces[p][0]])

    def first_way(p):
        (to_x if along_x_first(p) else to_y)(p, 0, 0)

    def second_way(p):
        (to_y if along_x_first(p) else to_x)(p, 0, 0)

    def send_early(p):
        src = wholes[pieces[p][0]].at[:, across(p)]
        if along_x_first(p):
            start(src, early.at[p], (x_next, col), sent_sem.at[3 + p], landing(p, 0, 1))
        else:
            start(src, early.at[p], (y_next, col), sent_sem.at[3 + p], landing(p, 1, 0))

    def landed_early(p, dy, dx):
        return pieces[p][4] and (dy, dx) == ((0, 1) if along_x_first(p) else (1, 0))

    def find_factor(p):
        unit = pieces[p][0]
        wait_bytes(peaks.at[unit, pl.ds(0, n_shard - 1), :, across(p)], peak_recv.at[p])
        factor = peaks[unit, 0, :, across(p)]
        for d in range(1, n_shard):
            factor = jnp.maximum(factor, peaks[unit, d, :, across(p)])
        factors[unit][:, across(p)] = factor

    def narrow(p, owner, read):
        unit = pieces[p][0]

        def step(i, carry):
            at = i * 16
            value = read(pl.ds(pl.multiple_of(at, 16), 16)) / factors[unit][:, across(p)]
            serves[unit][pl.ds(pl.multiple_of(owner * rows + at, 16), 16), across(p)] = value.astype(jnp.bfloat16)
            return carry

        lax.fori_loop(0, rows // 16, step, 0, unroll=2)

    def narrow_own(p):
        narrow(p, me, lambda span: wholes[pieces[p][0]][span, across(p)])

    def arrived(p, dy, dx):
        if landed_early(p, dy, dx):
            wait_bytes(early.at[p], landing(p, dy, dx))
            owner = (lax.rem(ypos - dy + ny, ny) * nx + lax.rem(xpos - dx + nx, nx)) * 2 + core
            narrow(p, owner, lambda span: early[p, span])
        else:
            wait_bytes(piece_of(p, dy, dx, core), landing(p, dy, dx))

    per = norm_train.shape[1]
    lead = min(first + 2, count)
    for p in range(lead):
        average(p)
    pl.semaphore_wait(barrier, n_shard + n_model - 2)
    for p in range(lead):
        send_peaks(p)
    for p in early_pieces:
        send_early(p)
    wait_bytes(norm_in, norm_load)
    norm_all[me, col, :, 0:per] = norm_in[0] + norm_in[1]
    for p in range(lead, count):
        average(p)
        if p > lead:
            send_peaks(p - 1)
    if count > lead:
        send_peaks(count - 1)
    for d in range(1, n_model):
        ref = norm_all.at[me, col]
        start(ref, ref, (me, lax.rem(col + d, n_model)), norm_send, norm_recv)

    late = list(range(first, count))
    for p in late[:2]:
        find_factor(p)
    for n, p in enumerate(late[:2]):
        narrow_own(p)
        if n < first:
            find_factor(n)
        first_way(p)
    for p in early_pieces[len(late[:2]):]:
        find_factor(p)
    wait_bytes(norm_all.at[0, pl.ds(0, n_model - 1)], norm_recv)
    for d in range(1, n_shard):
        start(norm_all.at[me], norm_all.at[me], (lax.rem(me + d, n_shard), col), row_send, row_recv)
    before = None
    for p in late[2:]:
        find_factor(p)
        if before is not None:
            first_way(before)
        narrow_own(p)
        before = p
    for p in early_pieces:
        narrow_own(p)
    if before is not None:
        first_way(before)
    for p in late + early_pieces:
        second_way(p)
    for p in order:
        to_pair(p, 0, 0)

    def gather_norm():
        wait_bytes(norm_all.at[pl.ds(0, n_shard - 1)], row_recv)
        lane = lax.broadcasted_iota(jnp.int32, (8, LANES), 1)
        tiles = [jnp.zeros((8, LANES), jnp.float32) for _ in range(norm_out.shape[0])]
        for s in range(n_shard):
            for c in range(n_model):
                for at in range(0, per, LANES):
                    size = min(LANES, per - at)
                    tile, shift = divmod((s * n_model + c) * per + at, LANES)
                    row = jnp.broadcast_to(norm_all[s, c, :, at:at + LANES], (8, LANES))
                    if shift:
                        row = pltpu.roll(row, shift, 1)
                    tiles[tile] = jnp.where((lane >= shift) & (lane < shift + size), row, tiles[tile])
                    if shift + size > LANES:
                        tiles[tile + 1] = jnp.where(lane < shift + size - LANES, row, tiles[tile + 1])
        for t, tile in enumerate(tiles):
            norm_rows[t:t + 1] = tile[0:1]
        norm_out[...] = norm_rows[...].astype(jnp.bfloat16)

    for distance in range(1, ny + nx - 1):
        for own_way in (True, False):
            for p in order:
                for dy in range(ny):
                    dx = distance - dy
                    straight = (dy if along_x_first(p) else dx) == 0
                    if 0 <= dx < nx and straight == own_way:
                        arrived(p, dy, dx)
                        to_x(p, dy, dx)
                        to_y(p, dy, dx)
                        to_pair(p, dy, dx)
            if distance == 1 and own_way:
                gather_norm()

    spread = first * LANES
    hops = 2 * ny * nx - 1
    for unit in range(2):
        wait_bytes(serves[unit].at[pl.ds(0, ny * nx * rows)], pair_recv.at[unit])
    wait_bytes(serve_gate.at[pl.ds(0, hops * rows), pl.ds(spread, cols - spread)], sent_sem.at[0])
    wait_bytes(serve_up.at[pl.ds(0, hops * rows)], sent_sem.at[1])
    if early_pieces:
        wait_bytes(serve_gate.at[pl.ds(0, (hops - 1) * rows), pl.ds(0, spread)], sent_sem.at[2])
    for p in early_pieces:
        wait_bytes(early.at[p], sent_sem.at[3 + p])
    wait_bytes(peaks.at[:, pl.ds(0, n_shard - 1)], peak_send)
    wait_bytes(norm_all.at[0, pl.ds(0, n_model - 1)], norm_send)
    wait_bytes(norm_all.at[pl.ds(0, n_shard - 1)], row_send)


def store_kernel(count, parts, *refs):
    pairs = list(zip(refs[:count], refs[count:-1]))
    for n, (src, dst) in enumerate(pairs):
        pieces = parts if src.shape[0] % (parts * 16) == 0 else 1
        size = src.shape[0] // pieces
        for part in range(pieces):
            span = pl.ds(part * size, size)
            pltpu.make_async_copy(src.at[span], dst.at[span], refs[-1].at[n]).start()
    for n, (src, dst) in enumerate(pairs):
        pltpu.make_async_copy(src, dst, refs[-1].at[n]).wait()


def store(arrays, parts):
    hbm = pl.BlockSpec(memory_space=pltpu.HBM)
    return pl.pallas_call(
        functools.partial(store_kernel, len(arrays), parts),
        out_shape=tuple(pltpu.HBM(a.shape, a.dtype) for a in arrays),
        in_specs=[pl.BlockSpec(memory_space=pltpu.VMEM)] * len(arrays),
        out_specs=(hbm,) * len(arrays),
        scratch_shapes=[pltpu.SemaphoreType.DMA((len(arrays),))],
        compiler_params=pltpu.CompilerParams(vmem_limit_bytes=1024 * 1024),
    )(*(pltpu.with_memory_space_constraint(a, pltpu.VMEM) for a in arrays))


def solution(mesh):
    n_shard, n_model = mesh.shape["shard"], mesh.shape["model"]
    ny, nx = grid_of(n_shard)

    def body(weight_gate, smooth_gate, weight_up, smooth_up, norm_train, norm_step):
        rows, cols = weight_gate.shape
        per = norm_train.shape[0]
        pieces = pieces_of(cols, min(nx, ny) > 1)
        count = len(pieces)
        wide = -(-per // LANES) * LANES
        width = n_shard * n_model * per
        tiles = -(-width // LANES)
        vmem = pl.BlockSpec(memory_space=pltpu.VMEM)
        hbm = pl.BlockSpec(memory_space=pltpu.HBM)
        dma = pltpu.SemaphoreType.DMA
        landed = pl.pallas_call(
            functools.partial(kernel, n_shard, n_model, ny, nx, pieces),
            out_shape=(
                pltpu.VMEM((n_shard * rows, cols), jnp.bfloat16),
                pltpu.VMEM((n_shard * rows, cols), jnp.bfloat16),
                pltpu.VMEM((1, cols), jnp.float32),
                pltpu.VMEM((1, cols), jnp.float32),
                pltpu.VMEM((tiles, LANES), jnp.bfloat16),
                pltpu.VMEM((rows, cols), jnp.float32),
                pltpu.VMEM((rows, cols), jnp.float32),
            ),
            in_specs=[hbm] * 6,
            out_specs=(vmem,) * 7,
            scratch_shapes=[
                pltpu.VMEM((2, 2, rows, cols), jnp.float32),
                pltpu.VMEM((2, n_shard, 1, cols), jnp.float32),
                pltpu.VMEM((2, rows, LANES), jnp.float32),
                pltpu.VMEM((2, 1, per), jnp.float32),
                pltpu.VMEM((n_shard, n_model, 1, wide), jnp.float32),
                pltpu.VMEM((tiles, LANES), jnp.float32),
                dma((count,)),
                dma((count,)),
                dma((count * (ny * nx - 1),)),
                dma((2,)),
                dma((5,)),
                dma((6,)),
            ],
            compiler_params=pltpu.CompilerParams(
                collective_id=0, has_side_effects=True, vmem_limit_bytes=20 * 1024 * 1024
            ),
        )(
            *(
                pltpu.with_memory_space_constraint(a, pltpu.HBM)
                for a in (weight_gate, smooth_gate, weight_up, smooth_up, norm_train[None], norm_step[None])
            ),
        )
        serve_gate, serve_up, factor_gate, factor_up, norm, whole_gate, whole_up = store(landed, 4)
        return (
            serve_gate, serve_up, factor_gate.reshape(-1), factor_up.reshape(-1),
            norm.reshape(-1)[:width], whole_gate, whole_up,
        )

    in_specs = (P("shard", "model"),) * 4 + (P(("shard", "model")),) * 2
    out_specs = (
        P(None, "model"),
        P(None, "model"),
        P("model"),
        P("model"),
        P(),
        P("shard", "model"),
        P("shard", "model"),
    )
    return jax.shard_map(body, mesh=mesh, in_specs=in_specs, out_specs=out_specs, check_vma=False)
```

```python
import functools
import math

import jax
import jax.numpy as jnp
from jax import lax
from jax.experimental import pallas as pl
from jax.experimental.pallas import tpu as pltpu
from jax.sharding import PartitionSpec as P

MESH = pl.DeviceIdType.MESH
keep_rate = 0.7
LANES = 128


def grid_of(n_shard):
    chips = n_shard // 2
    nx = math.isqrt(chips)
    while chips % nx:
        nx -= 1
    return chips // nx, nx


def pieces_of(cols, early):
    tiles = cols // LANES
    found = []
    for unit in range(2):
        queues = []
        for along_x, many in ((True, (tiles + 1) // 2), (False, tiles // 2)):
            if many < 3:
                widths = [1] * many
            else:
                widths = [1, 1, many - 2] if unit == 0 else [many - 1, 1]
            queues.append((along_x, widths))
        at = 0
        for n in range(max(len(q) for _, q in queues)):
            for along_x, widths in queues:
                if n < len(widths):
                    found.append((unit, at * LANES, widths[n] * LANES, along_x, early and unit == 0 and n == 1))
                    at += widths[n]
    return found


def spans_of(pieces):
    spans = []
    for unit, at, width, _, _ in pieces:
        if spans and spans[-1][0] == unit and spans[-1][2] + width <= 2 * LANES:
            spans[-1] = (unit, spans[-1][1], spans[-1][2] + width)
        else:
            spans.append((unit, at, width))
    return spans


def kernel(
    n_shard, n_model, ny, nx, pieces, spans,
    weight_gate, smooth_gate, weight_up, smooth_up, norm_train, norm_step,
    serve_gate, serve_up, factor_gate, factor_up, norm_out, whole_gate, whole_up,
    inputs, peaks, early, norm_in, norm_mine, norm_all, norm_rows,
    load_sem, peak_recv, ring_recv, second_recv, pair_recv, sent_sem, small_sem,
):
    me = lax.axis_index("shard")
    col = lax.axis_index("model")
    core = lax.rem(me, 2)
    chip = me // 2
    xpos, ypos = lax.rem(chip, nx), chip // nx
    x_next = (ypos * nx + lax.rem(xpos + 1, nx)) * 2 + core
    y_next = (lax.rem(ypos + 1, ny) * nx + xpos) * 2 + core
    pair = chip * 2 + (1 - core)
    rows, cols = whole_gate.shape
    serves, wholes, factors = (serve_gate, serve_up), (whole_gate, whole_up), (factor_gate, factor_up)
    order = range(len(pieces))
    early_pieces = [p for p in order if pieces[p][4]]
    lead = 1
    is_lead = me == lead
    per = norm_train.shape[1]
    norm_load, peak_send, mine_send, mine_recv, z_send, z_recv, all_send, all_recv = [small_sem.at[i] for i in range(8)]

    def across(p):
        return pl.ds(pieces[p][1], pieces[p][2])

    def wait_bytes(ref, sem):
        pltpu.make_async_copy(ref, ref, sem).wait()

    groups = [[], [], []]
    for p in order:
        groups[2 if pieces[p][0] else int(pieces[p][1] >= 2 * LANES)].append(p)
    reach = [(pieces[g[0]][0], pieces[g[0]][1], sum(pieces[p][2] for p in g)) for g in groups if g]
    groups = [g for g in groups if g]

    sources = ((weight_gate, smooth_gate), (weight_up, smooth_up))
    for n, (unit, at, width) in enumerate(spans):
        for which in range(2):
            pltpu.make_async_copy(
                sources[unit][which].at[:, pl.ds(at, width)], inputs.at[which, unit, :, pl.ds(at, width)], load_sem.at[n]
            ).start()
    for i, src in enumerate((norm_train, norm_step)):
        pltpu.make_async_copy(src, norm_in.at[i], norm_load).start()

    barrier = pltpu.get_barrier_semaphore()
    for d in range(1, n_shard):
        pl.semaphore_signal(barrier, inc=1, device_id=(lax.rem(me + d, n_shard), col), device_id_type=MESH)

    @pl.when(is_lead)
    def _():
        for d in range(1, n_model):
            pl.semaphore_signal(barrier, inc=1, device_id=(me, lax.rem(col + d, n_model)), device_id_type=MESH)

    def average(n):
        unit, first, width = spans[n]
        here = pl.ds(first, width)
        wait_bytes(inputs.at[:, unit, :, here], load_sem.at[n])

        def step(i, top):
            rows_now = pl.ds(pl.multiple_of(i * 8, 8), 8)
            value = keep_rate * inputs[1, unit, rows_now, here] + (1.0 - keep_rate) * inputs[0, unit, rows_now, here]
            wholes[unit][rows_now, here] = value
            return jnp.maximum(top, jnp.abs(value))

        top = lax.fori_loop(0, rows // 8, step, jnp.zeros((8, width), jnp.float32), unroll=4)
        peaks[unit, me, :, here] = jnp.max(top, axis=0, keepdims=True)

    def start(src, dst, device, send_sem, recv_sem):
        pltpu.make_async_remote_copy(
            src_ref=src, dst_ref=dst, send_sem=send_sem, recv_sem=recv_sem,
            device_id=device, device_id_type=MESH,
        ).start()

    def send_peaks(g):
        unit, at, width = reach[g]
        ref = peaks.at[unit, me, :, pl.ds(at, width)]
        for d in range(1, n_shard):
            start(ref, ref, (lax.rem(me + d, n_shard), col), peak_send, peak_recv.at[g])

    def piece_of(p, dy, dx, side):
        owner = (lax.rem(ypos - dy + ny, ny) * nx + lax.rem(xpos - dx + nx, nx)) * 2 + side
        return serves[pieces[p][0]].at[pl.ds(pl.multiple_of(owner * rows, rows), rows), across(p)]

    def group_of(p):
        return 2 if pieces[p][4] else pieces[p][0]

    def along_x_first(p):
        return pieces[p][3]

    def on_second_way(p, dy, dx):
        return (dy, dx) == ((1, 0) if along_x_first(p) else (0, 1))

    landings = [(p, dy, dx) for p in order for dy in range(ny) for dx in range(nx)]
    landings = [spot for spot in landings if spot[1:] != (0, 0) and not on_second_way(*spot)]

    def landing(p, dy, dx):
        if on_second_way(p, dy, dx):
            return second_recv.at[pieces[p][0]]
        return ring_recv.at[landings.index((p, dy, dx))]

    def to_x(p, dy, dx):
        if dx < nx - 1 and (dy == 0 or not along_x_first(p)):
            ref = piece_of(p, dy, dx, core)
            start(ref, ref, (x_next, col), sent_sem.at[group_of(p)], landing(p, dy, dx + 1))

    def to_y(p, dy, dx):
        if dy < ny - 1 and (dx == 0 or along_x_first(p)):
            ref = piece_of(p, dy, dx, core)
            start(ref, ref, (y_next, col), sent_sem.at[group_of(p)], landing(p, dy + 1, dx))

    def to_pair(p, dy, dx):
        ref = piece_of(p, dy, dx, core)
        start(ref, ref, (pair, col), sent_sem.at[group_of(p)], pair_recv.at[pieces[p][0]])

    def first_way(p):
        (to_x if along_x_first(p) else to_y)(p, 0, 0)

    def second_way(p):
        (to_y if along_x_first(p) else to_x)(p, 0, 0)

    chunks = 4 if rows % 32 == 0 else 1

    def send_early(chunk):
        span = pl.ds(chunk * (rows // chunks), rows // chunks)
        for n, p in enumerate(early_pieces):
            device, spot = (x_next, (0, 1)) if along_x_first(p) else (y_next, (1, 0))
            start(
                wholes[pieces[p][0]].at[span, across(p)], early.at[n, span], (device, col),
                sent_sem.at[3 + n], landing(p, *spot),
            )

    def landed_early(p, dy, dx):
        return pieces[p][4] and (dy, dx) == ((0, 1) if along_x_first(p) else (1, 0))

    def find_factor(g):
        unit, at, width = reach[g]
        here = pl.ds(at, width)
        wait_bytes(peaks.at[unit, pl.ds(0, n_shard - 1), :, here], peak_recv.at[g])
        factor = peaks[unit, 0, :, here]
        for d in range(1, n_shard):
            factor = jnp.maximum(factor, peaks[unit, d, :, here])
        factors[unit][:, here] = factor

    def narrow(p, owner, read):
        unit = pieces[p][0]

        def step(i, carry):
            at = i * 16
            value = read(pl.ds(pl.multiple_of(at, 16), 16)) / factors[unit][:, across(p)]
            serves[unit][pl.ds(pl.multiple_of(owner * rows + at, 16), 16), across(p)] = value.astype(jnp.bfloat16)
            return carry

        lax.fori_loop(0, rows // 16, step, 0, unroll=2)

    def narrow_own(p):
        narrow(p, me, lambda span: wholes[pieces[p][0]][span, across(p)])

    seconds = set()

    def arrived(p, dy, dx):
        if landed_early(p, dy, dx):
            n = early_pieces.index(p)
            wait_bytes(early.at[n], landing(p, dy, dx))
            owner = (lax.rem(ypos - dy + ny, ny) * nx + lax.rem(xpos - dx + nx, nx)) * 2 + core
            narrow(p, owner, lambda span: early[n, span])
        elif not on_second_way(p, dy, dx):
            wait_bytes(piece_of(p, dy, dx, core), landing(p, dy, dx))
        elif pieces[p][0] not in seconds:
            seconds.add(pieces[p][0])
            wait_bytes(serves[pieces[p][0]].at[pl.ds(0, rows)], landing(p, dy, dx))

    def norm_sum():
        wait_bytes(norm_in, norm_load)
        norm_mine[...] = jnp.zeros(norm_mine.shape, jnp.float32)
        norm_mine[:, 0:per] = norm_in[0] + norm_in[1]

    def norm_to_lead():
        @pl.when(jnp.logical_not(is_lead))
        def _():
            start(norm_mine, norm_all.at[col, me], (lead, col), mine_send, mine_recv)

    def norm_spread():
        @pl.when(is_lead)
        def _():
            norm_all[col, me] = norm_mine[...]
            wait_bytes(norm_all.at[0, pl.ds(0, n_shard - 1)], mine_recv)
            for d in range(1, n_model):
                start(norm_all.at[col], norm_all.at[col], (me, lax.rem(col + d, n_model)), z_send, z_recv)
            wait_bytes(norm_all.at[pl.ds(0, n_model - 1)], z_recv)
            for d in range(1, n_shard):
                start(norm_all, norm_all, (lax.rem(me + d, n_shard), col), all_send, all_recv)

    average(0)

    @pl.when(is_lead)
    def _():
        pl.semaphore_wait(barrier, n_shard + n_model - 2)

    @pl.when(jnp.logical_not(is_lead))
    def _():
        pl.semaphore_wait(barrier, n_shard - 1)

    ends = [at + width for _, at, width in reach]
    ready, chunk = 0, 0
    for n, (unit, at, width) in enumerate(spans):
        if n:
            average(n)
        if (unit, at + width) == (reach[ready][0], ends[ready]):
            send_peaks(ready)
            ready += 1
        if n and chunk < chunks:
            send_early(chunk)
            chunk += 1
    while chunk < chunks:
        send_early(chunk)
        chunk += 1

    for g, group in enumerate(groups):
        find_factor(g)
        before = None
        for p in [p for p in group if p not in early_pieces] + [p for p in group if p in early_pieces]:
            narrow_own(p)
            if before is not None:
                first_way(before)
            before = None if p in early_pieces else p
        if g == 0:
            norm_sum()
        if g == len(groups) - 1:
            for p in groups[0]:
                to_pair(p, 0, 0)
        if before is not None:
            first_way(before)
        if g == 0:
            norm_to_lead()
    norm_spread()
    for p in order:
        if p not in early_pieces:
            second_way(p)
    for p in early_pieces:
        second_way(p)
    for group in groups[1:]:
        for p in group:
            to_pair(p, 0, 0)

    def gather_norm():
        @pl.when(jnp.logical_not(is_lead))
        def _():
            wait_bytes(norm_all, all_recv)

        lane = lax.broadcasted_iota(jnp.int32, (8, LANES), 1)
        tiles = [jnp.zeros((8, LANES), jnp.float32) for _ in range(norm_out.shape[0])]
        for s in range(n_shard):
            for c in range(n_model):
                for at in range(0, per, LANES):
                    size = min(LANES, per - at)
                    tile, shift = divmod((s * n_model + c) * per + at, LANES)
                    row = jnp.broadcast_to(norm_all[c, s, :, at:at + LANES], (8, LANES))
                    if shift:
                        row = pltpu.roll(row, shift, 1)
                    tiles[tile] = jnp.where((lane >= shift) & (lane < shift + size), row, tiles[tile])
                    if shift + size > LANES:
                        tiles[tile + 1] = jnp.where(lane < shift + size - LANES, row, tiles[tile + 1])
        for t, tile in enumerate(tiles):
            norm_rows[t:t + 1] = tile[0:1]
        norm_out[...] = norm_rows[...].astype(jnp.bfloat16)

    for distance in range(1, ny + nx - 1):
        for own_way in (True, False):
            for p in order:
                for dy in range(ny):
                    dx = distance - dy
                    straight = (dy if along_x_first(p) else dx) == 0
                    if 0 <= dx < nx and straight == own_way:
                        arrived(p, dy, dx)
                        to_x(p, dy, dx)
                        to_y(p, dy, dx)
                        to_pair(p, dy, dx)
            if distance == 1 and own_way:
                gather_norm()

    spread = len(early_pieces) * LANES
    hops = 2 * ny * nx - 1
    for unit in range(2):
        wait_bytes(serves[unit].at[pl.ds(0, ny * nx * rows)], pair_recv.at[unit])
    wait_bytes(serve_gate.at[pl.ds(0, hops * rows), pl.ds(0, cols - spread)], sent_sem.at[0])
    wait_bytes(serve_up.at[pl.ds(0, hops * rows)], sent_sem.at[1])
    if early_pieces:
        wait_bytes(serve_gate.at[pl.ds(0, (hops - 1) * rows), pl.ds(0, spread)], sent_sem.at[2])
    for n in range(len(early_pieces)):
        wait_bytes(early.at[n], sent_sem.at[3 + n])
    wait_bytes(peaks.at[:, pl.ds(0, n_shard - 1)], peak_send)

    @pl.when(is_lead)
    def _():
        wait_bytes(norm_all.at[pl.ds(0, n_model - 1)], z_send)
        halves = (n_shard - 1) * math.prod(norm_all.shape) * 2
        wide = next(w for w in (LANES << k for k in range(16)) if halves // w <= n_shard * rows)
        wait_bytes(serve_gate.at[pl.ds(0, halves // wide), pl.ds(0, wide)], all_send)

    @pl.when(jnp.logical_not(is_lead))
    def _():
        wait_bytes(norm_mine, mine_send)


def store_kernel(count, parts, *refs):
    pairs = list(zip(refs[:count], refs[count:-1]))
    for n, (src, dst) in enumerate(pairs):
        pieces = parts if src.shape[0] % (parts * 16) == 0 else 1
        size = src.shape[0] // pieces
        for part in range(pieces):
            span = pl.ds(part * size, size)
            pltpu.make_async_copy(src.at[span], dst.at[span], refs[-1].at[n]).start()
    for n, (src, dst) in enumerate(pairs):
        pltpu.make_async_copy(src, dst, refs[-1].at[n]).wait()


def store(arrays, parts):
    hbm = pl.BlockSpec(memory_space=pltpu.HBM)
    return pl.pallas_call(
        functools.partial(store_kernel, len(arrays), parts),
        out_shape=tuple(pltpu.HBM(a.shape, a.dtype) for a in arrays),
        in_specs=[pl.BlockSpec(memory_space=pltpu.VMEM)] * len(arrays),
        out_specs=(hbm,) * len(arrays),
        scratch_shapes=[pltpu.SemaphoreType.DMA((len(arrays),))],
        compiler_params=pltpu.CompilerParams(vmem_limit_bytes=1024 * 1024),
    )(*(pltpu.with_memory_space_constraint(a, pltpu.VMEM) for a in arrays))


def solution(mesh):
    n_shard, n_model = mesh.shape["shard"], mesh.shape["model"]
    ny, nx = grid_of(n_shard)

    def body(weight_gate, smooth_gate, weight_up, smooth_up, norm_train, norm_step):
        rows, cols = weight_gate.shape
        per = norm_train.shape[0]
        pieces = pieces_of(cols, min(nx, ny) > 1)
        spans = spans_of(pieces)
        count = len(pieces)
        wide = -(-per // LANES) * LANES
        width = n_shard * n_model * per
        tiles = -(-width // LANES)
        vmem = pl.BlockSpec(memory_space=pltpu.VMEM)
        hbm = pl.BlockSpec(memory_space=pltpu.HBM)
        dma = pltpu.SemaphoreType.DMA
        landed = pl.pallas_call(
            functools.partial(kernel, n_shard, n_model, ny, nx, pieces, spans),
            out_shape=(
                pltpu.VMEM((n_shard * rows, cols), jnp.bfloat16),
                pltpu.VMEM((n_shard * rows, cols), jnp.bfloat16),
                pltpu.VMEM((1, cols), jnp.float32),
                pltpu.VMEM((1, cols), jnp.float32),
                pltpu.VMEM((tiles, LANES), jnp.bfloat16),
                pltpu.VMEM((rows, cols), jnp.float32),
                pltpu.VMEM((rows, cols), jnp.float32),
            ),
            in_specs=[hbm] * 6,
            out_specs=(vmem,) * 7,
            scratch_shapes=[
                pltpu.VMEM((2, 2, rows, cols), jnp.float32),
                pltpu.VMEM((2, n_shard, 1, cols), jnp.float32),
                pltpu.VMEM((2, rows, LANES), jnp.float32),
                pltpu.VMEM((2, 1, per), jnp.float32),
                pltpu.VMEM((1, wide), jnp.float32),
                pltpu.VMEM((n_model, n_shard, 1, wide), jnp.float32),
                pltpu.VMEM((tiles, LANES), jnp.float32),
                dma((len(spans),)),
                dma((3,)),
                dma((count * (ny * nx - 2),)),
                dma((2,)),
                dma((2,)),
                dma((5,)),
                dma((8,)),
            ],
            compiler_params=pltpu.CompilerParams(
                collective_id=0, has_side_effects=True, vmem_limit_bytes=20 * 1024 * 1024
            ),
        )(
            *(
                pltpu.with_memory_space_constraint(a, pltpu.HBM)
                for a in (weight_gate, smooth_gate, weight_up, smooth_up, norm_train[None], norm_step[None])
            ),
        )
        serve_gate, serve_up, factor_gate, factor_up, norm, whole_gate, whole_up = store(landed, 4)
        return (
            serve_gate, serve_up, factor_gate.reshape(-1), factor_up.reshape(-1),
            norm.reshape(-1)[:width], whole_gate, whole_up,
        )

    in_specs = (P("shard", "model"),) * 4 + (P(("shard", "model")),) * 2
    out_specs = (
        P(None, "model"),
        P(None, "model"),
        P("model"),
        P("model"),
        P(),
        P("shard", "model"),
        P("shard", "model"),
    )
    return jax.shard_map(body, mesh=mesh, in_specs=in_specs, out_specs=out_specs, check_vma=False)
```

```python
import functools
import math

import jax
import jax.numpy as jnp
from jax import lax
from jax.experimental import pallas as pl
from jax.experimental.pallas import tpu as pltpu
from jax.sharding import PartitionSpec as P

MESH = pl.DeviceIdType.MESH
keep_rate = 0.7
LANES = 128


def grid_of(n_shard):
    chips = n_shard // 2
    nx = math.isqrt(chips)
    while chips % nx:
        nx -= 1
    return chips // nx, nx


def pieces_of(rows, cols, ends):
    tiles = cols // LANES
    cut = rows * 3 // 4 // 16 * 16
    found, tails = [], []
    for unit in range(2):
        at = 0
        queues = []
        for along_x, many in ((True, (tiles + 1) // 2), (False, tiles // 2)):
            if many < 4 or not ends:
                queues.append([(along_x, 1, None)] * many)
            elif unit == 0:
                queues.append([(along_x, 2, None), (along_x, 1, "early"), (along_x, many - 3, None)])
            else:
                queues.append([(along_x, many - 1, None), (along_x, 1, "last")])
        for n in range(max(len(q) for q in queues)):
            for queue in queues:
                if n < len(queue):
                    along_x, width, kind = queue[n]
                    here = (unit, at * LANES, width * LANES)
                    at += width
                    if kind is None:
                        found.append(here + (0, rows, along_x, None))
                    else:
                        found.append(here + (0, cut, along_x, "early" if kind == "early" else None))
                        tails.append(here + (cut, rows - cut, along_x, "last" if kind == "last" else None))
        found += tails
        tails = []
    return found


def spans_of(pieces):
    spans = []
    for unit, at, width, top, _, _, _ in pieces:
        if top:
            continue
        if spans and spans[-1][0] == unit and spans[-1][2] == width and width <= 2 * LANES:
            spans[-1] = (unit, spans[-1][1], spans[-1][2] + width)
        else:
            spans.append((unit, at, width))
    return spans


def kernel(
    n_shard, n_model, ny, nx, pieces, spans,
    weight_gate, smooth_gate, weight_up, smooth_up, norm_train, norm_step,
    serve_gate, serve_up, factor_gate, factor_up, norm_out, whole_gate, whole_up,
    inputs, peaks, chip_peaks, early, norm_in, norm_mine, norm_all, norm_rows,
    load_sem, peak_send, peak_recv, couple_recv, ring_recv, second_recv, pair_recv, both_recv, sent_sem, small_sem,
):
    me = lax.axis_index("shard")
    col = lax.axis_index("model")
    core = lax.rem(me, 2)
    chip = me // 2
    xpos, ypos = lax.rem(chip, nx), chip // nx
    x_next = (ypos * nx + lax.rem(xpos + 1, nx)) * 2 + core
    y_next = (lax.rem(ypos + 1, ny) * nx + xpos) * 2 + core
    pair = chip * 2 + (1 - core)
    rows, cols = whole_gate.shape
    serves, wholes, factors = (serve_gate, serve_up), (whole_gate, whole_up), (factor_gate, factor_up)
    order = range(len(pieces))
    early_pieces = [p for p in order if pieces[p][6] == "early"]
    last_pieces = [p for p in order if pieces[p][6] == "last"]
    chips = ny * nx
    lead = 1
    is_lead = me == lead
    per = norm_train.shape[1]
    norm_load, mine_send, mine_recv, z_send, z_recv, all_send, all_recv = [small_sem.at[i] for i in range(7)]

    def across(p):
        return pl.ds(pieces[p][1], pieces[p][2])

    def wait_bytes(ref, sem):
        pltpu.make_async_copy(ref, ref, sem).wait()

    def blob(halves):
        wide = next(
            w for w in range(LANES, cols + 1, LANES) if halves % (8 * w) == 0 and halves // w <= n_shard * rows
        )
        return serve_gate.at[pl.ds(0, halves // wide), pl.ds(0, wide)]

    groups = [[], [], []]
    for p in order:
        unit, at = pieces[p][:2]
        groups[2 if unit else int(at >= sum(spans[0][1:]))].append(p)
    groups = [g for g in groups if g]
    reach = [
        (pieces[g[0]][0], pieces[g[0]][1], sum(pieces[p][2] for p in g if pieces[p][3] == 0)) for g in groups
    ]

    sources = ((weight_gate, smooth_gate), (weight_up, smooth_up))
    for n, (unit, at, width) in enumerate(spans):
        for which in range(2):
            pltpu.make_async_copy(
                sources[unit][which].at[:, pl.ds(at, width)], inputs.at[which, unit, :, pl.ds(at, width)], load_sem.at[n]
            ).start()
    for i, src in enumerate((norm_train, norm_step)):
        pltpu.make_async_copy(src, norm_in.at[i], norm_load).start()

    barrier = pltpu.get_barrier_semaphore()
    for d in range(1, n_shard):
        pl.semaphore_signal(barrier, inc=1, device_id=(lax.rem(me + d, n_shard), col), device_id_type=MESH)

    @pl.when(is_lead)
    def _():
        for d in range(1, n_model):
            pl.semaphore_signal(barrier, inc=1, device_id=(me, lax.rem(col + d, n_model)), device_id_type=MESH)

    def average(n):
        unit, first, width = spans[n]
        here = pl.ds(first, width)
        wait_bytes(inputs.at[:, unit, :, here], load_sem.at[n])

        def step(i, top):
            rows_now = pl.ds(pl.multiple_of(i * 8, 8), 8)
            value = keep_rate * inputs[1, unit, rows_now, here] + (1.0 - keep_rate) * inputs[0, unit, rows_now, here]
            wholes[unit][rows_now, here] = value
            return jnp.maximum(top, jnp.abs(value))

        top = lax.fori_loop(0, rows // 8, step, jnp.zeros((8, width), jnp.float32), unroll=4)
        peaks[unit, me, :, here] = jnp.max(top, axis=0, keepdims=True)

    def start(src, dst, device, send_sem, recv_sem):
        pltpu.make_async_remote_copy(
            src_ref=src, dst_ref=dst, send_sem=send_sem, recv_sem=recv_sem,
            device_id=device, device_id_type=MESH,
        ).start()

    def across_group(g):
        return pl.ds(reach[g][1], reach[g][2])

    def send_peaks(g):
        ref = peaks.at[reach[g][0], me, :, across_group(g)]
        if g == 0:
            for d in range(1, n_shard):
                start(ref, ref, (lax.rem(me + d, n_shard), col), peak_send.at[g], peak_recv.at[g])
        else:
            start(ref, ref, (pair, col), peak_send.at[g], couple_recv.at[g])

    def combine_peaks(g):
        unit, here = reach[g][0], across_group(g)
        wait_bytes(peaks.at[unit, 0, :, here], couple_recv.at[g])
        chip_peaks[unit, chip, :, here] = jnp.maximum(peaks[unit, me, :, here], peaks[unit, pair, :, here])

    def spread_peaks(g):
        ref = chip_peaks.at[reach[g][0], chip, :, across_group(g)]
        for d in range(1, chips):
            start(ref, ref, (lax.rem(me + 2 * d, n_shard), col), peak_send.at[g], peak_recv.at[g])

    def piece_of(p, dy, dx, side):
        owner = (lax.rem(ypos - dy + ny, ny) * nx + lax.rem(xpos - dx + nx, nx)) * 2 + side
        unit, _, _, top, height = pieces[p][:5]
        return serves[unit].at[pl.ds(pl.multiple_of(owner * rows + top, 16), height), across(p)]

    def along_x_first(p):
        return pieces[p][5]

    def on_second_way(p, dy, dx):
        return (dy, dx) == ((1, 0) if along_x_first(p) else (0, 1))

    landings = [(p, dy, dx) for p in order for dy in range(ny) for dx in range(nx)]
    landings = [spot for spot in landings if spot[1:] != (0, 0) and not on_second_way(*spot)]

    def landing(p, dy, dx):
        if on_second_way(p, dy, dx):
            return second_recv.at[pieces[p][0]]
        return ring_recv.at[landings.index((p, dy, dx))]

    sent = [0, 0, 0]
    paired = [0, 0]

    def send(p, spot, device, sem):
        ref = piece_of(p, *spot, core)
        kind = 2 if p in early_pieces else pieces[p][0]
        sent[kind] += pieces[p][2] * pieces[p][4]
        start(ref, ref, (device, col), sent_sem.at[kind], sem)

    def both_cores(p, dy, dx):
        return p in last_pieces and (dy, dx) == (ny - 1, nx - 1)

    def onward(p, spot, device, there):
        send(p, spot, device, landing(p, *there))
        if both_cores(p, *there):
            send(p, spot, device + 1 - 2 * core, both_recv.at[last_pieces.index(p)])

    def to_x(p, dy, dx):
        if dx < nx - 1 and (dy == 0 or not along_x_first(p)):
            onward(p, (dy, dx), x_next, (dy, dx + 1))

    def to_y(p, dy, dx):
        if dy < ny - 1 and (dx == 0 or along_x_first(p)):
            onward(p, (dy, dx), y_next, (dy + 1, dx))

    def to_pair(p, dy, dx):
        if not both_cores(p, dy, dx):
            paired[pieces[p][0]] += pieces[p][2] * pieces[p][4]
            send(p, (dy, dx), pair, pair_recv.at[pieces[p][0]])

    def first_way(p):
        (to_x if along_x_first(p) else to_y)(p, 0, 0)

    def second_way(p):
        (to_y if along_x_first(p) else to_x)(p, 0, 0)

    cut = pieces[early_pieces[0]][4] if early_pieces else 0
    chunks = 3 if cut % 24 == 0 else 1

    def send_early(chunk):
        span = pl.ds(chunk * (cut // chunks), cut // chunks)
        for n, p in enumerate(early_pieces):
            device, spot = (x_next, (0, 1)) if along_x_first(p) else (y_next, (1, 0))
            start(
                wholes[pieces[p][0]].at[span, across(p)], early.at[n, span], (device, col),
                sent_sem.at[3 + n], landing(p, *spot),
            )

    def landed_early(p, dy, dx):
        return p in early_pieces and (dy, dx) == ((0, 1) if along_x_first(p) else (1, 0))

    def find_factor(g):
        unit, here = reach[g][0], across_group(g)
        table, many = (peaks, n_shard) if g == 0 else (chip_peaks, chips)
        if many > 1:
            wait_bytes(table.at[unit, pl.ds(0, many - 1), :, here], peak_recv.at[g])
        factor = table[unit, 0, :, here]
        for d in range(1, many):
            factor = jnp.maximum(factor, table[unit, d, :, here])
        factors[unit][:, here] = factor

    def narrow(p, owner, read):
        unit, _, _, top, height = pieces[p][:5]

        def step(i, carry):
            at = top + i * 16
            value = read(pl.ds(pl.multiple_of(at, 16), 16)) / factors[unit][:, across(p)]
            serves[unit][pl.ds(pl.multiple_of(owner * rows + at, 16), 16), across(p)] = value.astype(jnp.bfloat16)
            return carry

        lax.fori_loop(0, height // 16, step, 0, unroll=2)

    def narrow_own(p):
        narrow(p, me, lambda span: wholes[pieces[p][0]][span, across(p)])

    seconds = set()

    def arrived(p, dy, dx):
        if landed_early(p, dy, dx):
            n = early_pieces.index(p)
            wait_bytes(early.at[n, pl.ds(0, cut)], landing(p, dy, dx))
            owner = (lax.rem(ypos - dy + ny, ny) * nx + lax.rem(xpos - dx + nx, nx)) * 2 + core
            narrow(p, owner, lambda span: early[n, span])
        elif not on_second_way(p, dy, dx):
            wait_bytes(piece_of(p, dy, dx, core), landing(p, dy, dx))
        elif pieces[p][0] not in seconds:
            seconds.add(pieces[p][0])
            wait_bytes(serves[pieces[p][0]].at[pl.ds(0, rows)], landing(p, dy, dx))

    def norm_sum():
        wait_bytes(norm_in, norm_load)
        norm_mine[...] = jnp.zeros(norm_mine.shape, jnp.float32)
        norm_mine[:, 0:per] = norm_in[0] + norm_in[1]

    def norm_to_lead():
        @pl.when(jnp.logical_not(is_lead))
        def _():
            start(norm_mine, norm_all.at[col, me], (lead, col), mine_send, mine_recv)

    def norm_spread():
        @pl.when(is_lead)
        def _():
            norm_all[col, me] = norm_mine[...]
            wait_bytes(norm_all.at[0, pl.ds(0, n_shard - 1)], mine_recv)
            for d in range(1, n_model):
                start(norm_all.at[col], norm_all.at[col], (me, lax.rem(col + d, n_model)), z_send, z_recv)
            wait_bytes(norm_all.at[pl.ds(0, n_model - 1)], z_recv)
            for d in range(1, n_shard):
                start(norm_all, norm_all, (lax.rem(me + d, n_shard), col), all_send, all_recv)

    average(0)

    @pl.when(is_lead)
    def _():
        pl.semaphore_wait(barrier, n_shard + n_model - 2)

    @pl.when(jnp.logical_not(is_lead))
    def _():
        pl.semaphore_wait(barrier, n_shard - 1)

    ready, chunk = 0, 0
    for n, (unit, at, width) in enumerate(spans):
        final = n == len(spans) - 1
        if final and ready > 1:
            combine_peaks(1)
        if n:
            average(n)
        if (unit, at + width) == (reach[ready][0], sum(reach[ready][1:])):
            send_peaks(ready)
            ready += 1
        if n and chunk < chunks and early_pieces:
            send_early(chunk)
            chunk += 1
    if len(groups) > 1:
        spread_peaks(1)

    for g, group in enumerate(groups):
        find_factor(g)
        before = None
        for p in [p for p in group if p not in early_pieces] + [p for p in group if p in early_pieces]:
            narrow_own(p)
            if before is not None:
                first_way(before)
            before = None if p in early_pieces else p
        if g == 0:
            norm_sum()
        if g == len(groups) - 1:
            for p in groups[0]:
                to_pair(p, 0, 0)
        if before is not None:
            first_way(before)
        if g == 0:
            for later in range(2, len(groups)):
                combine_peaks(later)
            norm_to_lead()
            for later in range(2, len(groups)):
                spread_peaks(later)
    norm_spread()
    for p in order:
        if p not in early_pieces:
            second_way(p)
    for p in early_pieces:
        second_way(p)
    for group in groups[1:]:
        for p in group:
            to_pair(p, 0, 0)

    def gather_norm():
        @pl.when(jnp.logical_not(is_lead))
        def _():
            wait_bytes(norm_all, all_recv)

        lane = lax.broadcasted_iota(jnp.int32, (8, LANES), 1)
        tiles = [jnp.zeros((8, LANES), jnp.float32) for _ in range(norm_out.shape[0])]
        for s in range(n_shard):
            for c in range(n_model):
                for at in range(0, per, LANES):
                    size = min(LANES, per - at)
                    tile, shift = divmod((s * n_model + c) * per + at, LANES)
                    row = jnp.broadcast_to(norm_all[c, s, :, at:at + LANES], (8, LANES))
                    if shift:
                        row = pltpu.roll(row, shift, 1)
                    tiles[tile] = jnp.where((lane >= shift) & (lane < shift + size), row, tiles[tile])
                    if shift + size > LANES:
                        tiles[tile + 1] = jnp.where(lane < shift + size - LANES, row, tiles[tile + 1])
        for t, tile in enumerate(tiles):
            norm_rows[t:t + 1] = tile[0:1]
        norm_out[...] = norm_rows[...].astype(jnp.bfloat16)

    for distance in range(1, ny + nx - 1):
        for own_way in (True, False):
            for p in order:
                for dy in range(ny):
                    dx = distance - dy
                    straight = (dy if along_x_first(p) else dx) == 0
                    if 0 <= dx < nx and straight == own_way:
                        arrived(p, dy, dx)
                        to_x(p, dy, dx)
                        to_y(p, dy, dx)
                        to_pair(p, dy, dx)
            if distance == 1 and own_way:
                gather_norm()

    for unit in range(2):
        wait_bytes(blob(paired[unit]), pair_recv.at[unit])
    for n, p in enumerate(last_pieces):
        wait_bytes(piece_of(p, ny - 1, nx - 1, 1 - core), both_recv.at[n])
    for kind, halves in enumerate(sent):
        if halves:
            wait_bytes(blob(halves), sent_sem.at[kind])
    for n in range(len(early_pieces)):
        wait_bytes(early.at[n, pl.ds(0, cut)], sent_sem.at[3 + n])
    wait_bytes(peaks.at[0, pl.ds(0, n_shard - 1), :, across_group(0)], peak_send.at[0])
    for g in range(1, len(groups)):
        wait_bytes(chip_peaks.at[reach[g][0], :, :, across_group(g)], peak_send.at[g])

    @pl.when(is_lead)
    def _():
        wait_bytes(norm_all.at[pl.ds(0, n_model - 1)], z_send)
        wait_bytes(blob((n_shard - 1) * math.prod(norm_all.shape) * 2), all_send)

    @pl.when(jnp.logical_not(is_lead))
    def _():
        wait_bytes(norm_mine, mine_send)


def store_kernel(count, parts, *refs):
    pairs = list(zip(refs[:count], refs[count:-1]))
    for n, (src, dst) in enumerate(pairs):
        pieces = parts if src.shape[0] % (parts * 16) == 0 else 1
        size = src.shape[0] // pieces
        for part in range(pieces):
            span = pl.ds(part * size, size)
            pltpu.make_async_copy(src.at[span], dst.at[span], refs[-1].at[n]).start()
    for n, (src, dst) in enumerate(pairs):
        pltpu.make_async_copy(src, dst, refs[-1].at[n]).wait()


def store(arrays, parts):
    hbm = pl.BlockSpec(memory_space=pltpu.HBM)
    return pl.pallas_call(
        functools.partial(store_kernel, len(arrays), parts),
        out_shape=tuple(pltpu.HBM(a.shape, a.dtype) for a in arrays),
        in_specs=[pl.BlockSpec(memory_space=pltpu.VMEM)] * len(arrays),
        out_specs=(hbm,) * len(arrays),
        scratch_shapes=[pltpu.SemaphoreType.DMA((len(arrays),))],
        compiler_params=pltpu.CompilerParams(vmem_limit_bytes=1024 * 1024),
    )(*(pltpu.with_memory_space_constraint(a, pltpu.VMEM) for a in arrays))


def solution(mesh):
    n_shard, n_model = mesh.shape["shard"], mesh.shape["model"]
    ny, nx = grid_of(n_shard)

    def body(weight_gate, smooth_gate, weight_up, smooth_up, norm_train, norm_step):
        rows, cols = weight_gate.shape
        per = norm_train.shape[0]
        pieces = pieces_of(rows, cols, min(nx, ny) > 1)
        spans = spans_of(pieces)
        count = len(pieces)
        wide = -(-per // LANES) * LANES
        width = n_shard * n_model * per
        tiles = -(-width // LANES)
        vmem = pl.BlockSpec(memory_space=pltpu.VMEM)
        hbm = pl.BlockSpec(memory_space=pltpu.HBM)
        dma = pltpu.SemaphoreType.DMA
        landed = pl.pallas_call(
            functools.partial(kernel, n_shard, n_model, ny, nx, pieces, spans),
            out_shape=(
                pltpu.VMEM((n_shard * rows, cols), jnp.bfloat16),
                pltpu.VMEM((n_shard * rows, cols), jnp.bfloat16),
                pltpu.VMEM((1, cols), jnp.float32),
                pltpu.VMEM((1, cols), jnp.float32),
                pltpu.VMEM((tiles, LANES), jnp.bfloat16),
                pltpu.VMEM((rows, cols), jnp.float32),
                pltpu.VMEM((rows, cols), jnp.float32),
            ),
            in_specs=[hbm] * 6,
            out_specs=(vmem,) * 7,
            scratch_shapes=[
                pltpu.VMEM((2, 2, rows, cols), jnp.float32),
                pltpu.VMEM((2, n_shard, 1, cols), jnp.float32),
                pltpu.VMEM((2, ny * nx, 1, cols), jnp.float32),
                pltpu.VMEM((2, rows, LANES), jnp.float32),
                pltpu.VMEM((2, 1, per), jnp.float32),
                pltpu.VMEM((1, wide), jnp.float32),
                pltpu.VMEM((n_model, n_shard, 1, wide), jnp.float32),
                pltpu.VMEM((tiles, LANES), jnp.float32),
                dma((len(spans),)),
                dma((3,)),
                dma((3,)),
                dma((3,)),
                dma((count * (ny * nx - 2),)),
                dma((2,)),
                dma((2,)),
                dma((2,)),
                dma((5,)),
                dma((7,)),
            ],
            compiler_params=pltpu.CompilerParams(
                collective_id=0, has_side_effects=True, vmem_limit_bytes=20 * 1024 * 1024
            ),
        )(
            *(
                pltpu.with_memory_space_constraint(a, pltpu.HBM)
                for a in (weight_gate, smooth_gate, weight_up, smooth_up, norm_train[None], norm_step[None])
            ),
        )
        serve_gate, serve_up, factor_gate, factor_up, norm, whole_gate, whole_up = store(landed, 4)
        return (
            serve_gate, serve_up, factor_gate.reshape(-1), factor_up.reshape(-1),
            norm.reshape(-1)[:width], whole_gate, whole_up,
        )

    in_specs = (P("shard", "model"),) * 4 + (P(("shard", "model")),) * 2
    out_specs = (
        P(None, "model"),
        P(None, "model"),
        P("model"),
        P("model"),
        P(),
        P("shard", "model"),
        P("shard", "model"),
    )
    return jax.shard_map(body, mesh=mesh, in_specs=in_specs, out_specs=out_specs, check_vma=False)
```

```python
import functools
import math

import jax
import jax.numpy as jnp
from jax import lax
from jax.experimental import pallas as pl
from jax.experimental.pallas import tpu as pltpu
from jax.sharding import PartitionSpec as P

MESH = pl.DeviceIdType.MESH
keep_rate = 0.7
LANES = 128


def grid_of(n_shard):
    chips = n_shard // 2
    nx = math.isqrt(chips)
    while chips % nx:
        nx -= 1
    return chips // nx, nx


def pieces_of(rows, cols, ends):
    tiles = cols // LANES
    cut = rows * 3 // 4 // 16 * 16
    found, tails = [], []
    for unit in range(2):
        at = 0
        queues = []
        for along_x, many in ((True, (tiles + 1) // 2), (False, tiles // 2)):
            if many < 4 or not ends:
                queues.append([(along_x, 1, None)] * many)
            elif unit == 0:
                queues.append([(along_x, 2, None), (along_x, 1, "early"), (along_x, many - 3, None)])
            else:
                near = many // 2
                queues.append([(along_x, near, "near"), (along_x, many - near - 1, None), (along_x, 1, "last")])
        for n in range(max(len(q) for q in queues)):
            for queue in queues:
                if n < len(queue):
                    along_x, width, kind = queue[n]
                    here = (unit, at * LANES, width * LANES)
                    at += width
                    if kind in (None, "near"):
                        found.append(here + (0, rows, along_x, kind))
                    else:
                        found.append(here + (0, cut, along_x, "early" if kind == "early" else None))
                        tails.append(here + (cut, rows - cut, along_x, "last" if kind == "last" else None))
        found += tails
        tails = []
    return found


def spans_of(pieces):
    spans = []
    for unit, at, width, top, _, _, _ in pieces:
        if top:
            continue
        if spans and spans[-1][0] == unit and spans[-1][2] == width and width <= 2 * LANES:
            spans[-1] = (unit, spans[-1][1], spans[-1][2] + width)
        else:
            spans.append((unit, at, width))
    return spans


def kernel(
    n_shard, n_model, ny, nx, pieces, spans,
    weight_gate, smooth_gate, weight_up, smooth_up, norm_train, norm_step,
    serve_gate, serve_up, factor_gate, factor_up, norm_out, whole_gate, whole_up, block,
    inputs, peaks, chip_peaks, early, norm_in, norm_mine, norm_all, norm_rows,
    load_sem, peak_send, peak_recv, couple_recv, ring_recv, second_recv, pair_recv, both_recv, sent_sem, small_sem,
):
    me = lax.axis_index("shard")
    col = lax.axis_index("model")
    core = lax.rem(me, 2)
    chip = me // 2
    xpos, ypos = lax.rem(chip, nx), chip // nx
    x_next = (ypos * nx + lax.rem(xpos + 1, nx)) * 2 + core
    y_next = (lax.rem(ypos + 1, ny) * nx + xpos) * 2 + core
    pair = chip * 2 + (1 - core)
    rows, cols = whole_gate.shape
    serves, wholes, factors = (serve_gate, serve_up), (whole_gate, whole_up), (factor_gate, factor_up)
    order = range(len(pieces))
    early_pieces = [p for p in order if pieces[p][6] == "early"]
    last_pieces = [p for p in order if pieces[p][6] == "last"]
    near_pieces = [p for p in order if pieces[p][6] == "near"]
    far = (ny - 1, nx - 1)
    chips = ny * nx
    lead = 1
    is_lead = me == lead
    per = norm_train.shape[1]
    norm_load, mine_send, mine_recv, z_send, z_recv, all_send, all_recv = [small_sem.at[i] for i in range(7)]

    def across(p):
        return pl.ds(pieces[p][1], pieces[p][2])

    def wait_bytes(ref, sem):
        pltpu.make_async_copy(ref, ref, sem).wait()

    def blob(halves):
        wide = next(
            w for w in range(LANES, cols + 1, LANES) if halves % (8 * w) == 0 and halves // w <= n_shard * rows
        )
        return serve_gate.at[pl.ds(0, halves // wide), pl.ds(0, wide)]

    groups = [[], [], []]
    for p in order:
        unit, at = pieces[p][:2]
        groups[2 if unit else int(at >= sum(spans[0][1:]))].append(p)
    groups = [g for g in groups if g]
    reach = [
        (pieces[g[0]][0], pieces[g[0]][1], sum(pieces[p][2] for p in g if pieces[p][3] == 0)) for g in groups
    ]

    sources = ((weight_gate, smooth_gate), (weight_up, smooth_up))
    for n, (unit, at, width) in enumerate(spans):
        for which in range(2):
            pltpu.make_async_copy(
                sources[unit][which].at[:, pl.ds(at, width)], inputs.at[which, unit, :, pl.ds(at, width)], load_sem.at[n]
            ).start()
    for i, src in enumerate((norm_train, norm_step)):
        pltpu.make_async_copy(src, norm_in.at[i], norm_load).start()

    barrier = pltpu.get_barrier_semaphore()
    for d in range(1, n_shard):
        pl.semaphore_signal(barrier, inc=1, device_id=(lax.rem(me + d, n_shard), col), device_id_type=MESH)

    @pl.when(is_lead)
    def _():
        for d in range(1, n_model):
            pl.semaphore_signal(barrier, inc=1, device_id=(me, lax.rem(col + d, n_model)), device_id_type=MESH)

    def average(n):
        unit, first, width = spans[n]
        here = pl.ds(first, width)
        wait_bytes(inputs.at[:, unit, :, here], load_sem.at[n])

        def step(i, top):
            rows_now = pl.ds(pl.multiple_of(i * 8, 8), 8)
            value = keep_rate * inputs[1, unit, rows_now, here] + (1.0 - keep_rate) * inputs[0, unit, rows_now, here]
            wholes[unit][rows_now, here] = value
            return jnp.maximum(top, jnp.abs(value))

        top = lax.fori_loop(0, rows // 8, step, jnp.zeros((8, width), jnp.float32), unroll=4)
        peaks[unit, me, :, here] = jnp.max(top, axis=0, keepdims=True)

    def start(src, dst, device, send_sem, recv_sem):
        pltpu.make_async_remote_copy(
            src_ref=src, dst_ref=dst, send_sem=send_sem, recv_sem=recv_sem,
            device_id=device, device_id_type=MESH,
        ).start()

    def across_group(g):
        return pl.ds(reach[g][1], reach[g][2])

    def send_peaks(g):
        ref = peaks.at[reach[g][0], me, :, across_group(g)]
        if g == 0:
            for d in range(1, n_shard):
                start(ref, ref, (lax.rem(me + d, n_shard), col), peak_send.at[g], peak_recv.at[g])
        else:
            start(ref, ref, (pair, col), peak_send.at[g], couple_recv.at[g])

    def combine_peaks(g):
        unit, here = reach[g][0], across_group(g)
        wait_bytes(peaks.at[unit, 0, :, here], couple_recv.at[g])
        chip_peaks[unit, chip, :, here] = jnp.maximum(peaks[unit, me, :, here], peaks[unit, pair, :, here])

    def spread_peaks(g):
        ref = chip_peaks.at[reach[g][0], chip, :, across_group(g)]
        for d in range(1, chips):
            start(ref, ref, (lax.rem(me + 2 * d, n_shard), col), peak_send.at[g], peak_recv.at[g])

    def piece_of(p, dy, dx, side):
        owner = (lax.rem(ypos - dy + ny, ny) * nx + lax.rem(xpos - dx + nx, nx)) * 2 + side
        unit, _, _, top, height = pieces[p][:5]
        return serves[unit].at[pl.ds(pl.multiple_of(owner * rows + top, 16), height), across(p)]

    def along_x_first(p):
        return pieces[p][5]

    def on_second_way(p, dy, dx):
        return (dy, dx) == ((1, 0) if along_x_first(p) else (0, 1))

    landings = [(p, dy, dx) for p in order for dy in range(ny) for dx in range(nx)]
    landings = [spot for spot in landings if spot[1:] != (0, 0) and not on_second_way(*spot)]
    landings = [spot for spot in landings if not (spot[0] in near_pieces and spot[1:] == far)]

    def landing(p, dy, dx):
        if on_second_way(p, dy, dx):
            return second_recv.at[pieces[p][0]]
        return ring_recv.at[landings.index((p, dy, dx))]

    sent = [0, 0, 0]
    paired = [0, 0, 0]

    def send(p, spot, device, sem):
        ref = piece_of(p, *spot, core)
        kind = 2 if p in early_pieces else pieces[p][0]
        sent[kind] += pieces[p][2] * pieces[p][4]
        start(ref, ref, (device, col), sent_sem.at[kind], sem)

    def both_cores(p, dy, dx):
        return p in last_pieces and (dy, dx) == far

    def onward(p, spot, device, there):
        if p in near_pieces and there == far:
            return
        send(p, spot, device, landing(p, *there))
        if both_cores(p, *there):
            send(p, spot, device + 1 - 2 * core, both_recv.at[last_pieces.index(p)])

    def to_x(p, dy, dx):
        if dx < nx - 1 and (dy == 0 or not along_x_first(p)):
            onward(p, (dy, dx), x_next, (dy, dx + 1))

    def to_y(p, dy, dx):
        if dy < ny - 1 and (dx == 0 or along_x_first(p)):
            onward(p, (dy, dx), y_next, (dy + 1, dx))

    def to_pair(p, dy, dx):
        if not both_cores(p, dy, dx):
            kind = 2 if p in near_pieces else pieces[p][0]
            paired[kind] += pieces[p][2] * pieces[p][4]
            send(p, (dy, dx), pair, pair_recv.at[kind])

    def first_way(p):
        (to_x if along_x_first(p) else to_y)(p, 0, 0)

    def second_way(p):
        (to_y if along_x_first(p) else to_x)(p, 0, 0)

    cut = pieces[early_pieces[0]][4] if early_pieces else 0
    chunks = 3 if cut % 24 == 0 else 1

    def send_early(chunk):
        span = pl.ds(chunk * (cut // chunks), cut // chunks)
        for n, p in enumerate(early_pieces):
            device, spot = (x_next, (0, 1)) if along_x_first(p) else (y_next, (1, 0))
            start(
                wholes[pieces[p][0]].at[span, across(p)], early.at[n, span], (device, col),
                sent_sem.at[3 + n], landing(p, *spot),
            )

    def landed_early(p, dy, dx):
        return p in early_pieces and (dy, dx) == ((0, 1) if along_x_first(p) else (1, 0))

    def find_factor(g):
        unit, here = reach[g][0], across_group(g)
        table, many = (peaks, n_shard) if g == 0 else (chip_peaks, chips)
        if many > 1:
            wait_bytes(table.at[unit, pl.ds(0, many - 1), :, here], peak_recv.at[g])
        factor = table[unit, 0, :, here]
        for d in range(1, many):
            factor = jnp.maximum(factor, table[unit, d, :, here])
        factors[unit][:, here] = factor

    def narrow(p, owner, read):
        unit, _, _, top, height = pieces[p][:5]

        def step(i, carry):
            at = top + i * 16
            value = read(pl.ds(pl.multiple_of(at, 16), 16)) / factors[unit][:, across(p)]
            serves[unit][pl.ds(pl.multiple_of(owner * rows + at, 16), 16), across(p)] = value.astype(jnp.bfloat16)
            return carry

        lax.fori_loop(0, height // 16, step, 0, unroll=2)

    def narrow_own(p):
        narrow(p, me, lambda span: wholes[pieces[p][0]][span, across(p)])

    seconds = set()

    def arrived(p, dy, dx):
        if landed_early(p, dy, dx):
            n = early_pieces.index(p)
            wait_bytes(early.at[n, pl.ds(0, cut)], landing(p, dy, dx))
            owner = (lax.rem(ypos - dy + ny, ny) * nx + lax.rem(xpos - dx + nx, nx)) * 2 + core
            narrow(p, owner, lambda span: early[n, span])
        elif not on_second_way(p, dy, dx):
            wait_bytes(piece_of(p, dy, dx, core), landing(p, dy, dx))
        elif pieces[p][0] not in seconds:
            seconds.add(pieces[p][0])
            wait_bytes(serves[pieces[p][0]].at[pl.ds(0, rows)], landing(p, dy, dx))

    def norm_sum():
        wait_bytes(norm_in, norm_load)
        norm_mine[...] = jnp.zeros(norm_mine.shape, jnp.float32)
        norm_mine[:, 0:per] = norm_in[0] + norm_in[1]

    def norm_to_lead():
        @pl.when(jnp.logical_not(is_lead))
        def _():
            start(norm_mine, norm_all.at[col, me], (lead, col), mine_send, mine_recv)

    def norm_spread():
        @pl.when(is_lead)
        def _():
            norm_all[col, me] = norm_mine[...]
            wait_bytes(norm_all.at[0, pl.ds(0, n_shard - 1)], mine_recv)
            for d in range(1, n_model):
                start(norm_all.at[col], norm_all.at[col], (me, lax.rem(col + d, n_model)), z_send, z_recv)
            wait_bytes(norm_all.at[pl.ds(0, n_model - 1)], z_recv)
            for d in range(1, n_shard):
                start(norm_all, norm_all, (lax.rem(me + d, n_shard), col), all_send, all_recv)

    average(0)

    @pl.when(is_lead)
    def _():
        pl.semaphore_wait(barrier, n_shard + n_model - 2)

    @pl.when(jnp.logical_not(is_lead))
    def _():
        pl.semaphore_wait(barrier, n_shard - 1)

    ready, chunk = 0, 0
    for n, (unit, at, width) in enumerate(spans):
        final = n == len(spans) - 1
        if final and ready > 1:
            combine_peaks(1)
        if n:
            average(n)
        if (unit, at + width) == (reach[ready][0], sum(reach[ready][1:])):
            send_peaks(ready)
            ready += 1
        if n and chunk < chunks and early_pieces:
            send_early(chunk)
            chunk += 1
    if len(groups) > 1:
        spread_peaks(1)

    for g, group in enumerate(groups):
        find_factor(g)
        before = None
        for p in [p for p in group if p not in early_pieces] + [p for p in group if p in early_pieces]:
            narrow_own(p)
            if before is not None:
                first_way(before)
            before = None if p in early_pieces else p
        if g == 0:
            norm_sum()
        if g == len(groups) - 1:
            for p in groups[0]:
                to_pair(p, 0, 0)
        if before is not None:
            first_way(before)
        if g == 0:
            for later in range(2, len(groups)):
                combine_peaks(later)
            norm_to_lead()
            for later in range(2, len(groups)):
                spread_peaks(later)
    norm_spread()
    for p in order:
        if p not in early_pieces:
            second_way(p)
    for p in early_pieces:
        second_way(p)
    for group in groups[1:]:
        for p in group:
            to_pair(p, 0, 0)

    def gather_norm():
        @pl.when(jnp.logical_not(is_lead))
        def _():
            wait_bytes(norm_all, all_recv)

        lane = lax.broadcasted_iota(jnp.int32, (8, LANES), 1)
        tiles = [jnp.zeros((8, LANES), jnp.float32) for _ in range(norm_out.shape[0])]
        for s in range(n_shard):
            for c in range(n_model):
                for at in range(0, per, LANES):
                    size = min(LANES, per - at)
                    tile, shift = divmod((s * n_model + c) * per + at, LANES)
                    row = jnp.broadcast_to(norm_all[c, s, :, at:at + LANES], (8, LANES))
                    if shift:
                        row = pltpu.roll(row, shift, 1)
                    tiles[tile] = jnp.where((lane >= shift) & (lane < shift + size), row, tiles[tile])
                    if shift + size > LANES:
                        tiles[tile + 1] = jnp.where(lane < shift + size - LANES, row, tiles[tile + 1])
        for t, tile in enumerate(tiles):
            norm_rows[t:t + 1] = tile[0:1]
        norm_out[...] = norm_rows[...].astype(jnp.bfloat16)

    def fill_block():
        wait_bytes(blob(paired[2]), pair_recv.at[2])
        chosen = lax.rem(ypos + 1 + core, ny) * nx + lax.rem(xpos + 2 - core, nx)
        base = 2 * rows * chosen
        width = block.shape[1]
        for c in range(2):
            @pl.when(core == c)
            def _():
                def step(i, carry):
                    block[pl.ds(pl.multiple_of(i * 16, 16), 16)] = serve_up[
                        pl.ds(pl.multiple_of(base + i * 16, 16), 16), c * width:(c + 1) * width
                    ]
                    return carry

                lax.fori_loop(0, 2 * rows // 16, step, 0, unroll=4)

    block_due = bool(near_pieces)
    for distance in range(1, ny + nx - 1):
        for own_way in (True, False):
            for p in order:
                for dy in range(ny):
                    dx = distance - dy
                    straight = (dy if along_x_first(p) else dx) == 0
                    if p in near_pieces and (dy, dx) == far:
                        continue
                    if 0 <= dx < nx and straight == own_way:
                        arrived(p, dy, dx)
                        to_x(p, dy, dx)
                        to_y(p, dy, dx)
                        to_pair(p, dy, dx)
                        if block_due and (dy, dx) == far:
                            block_due = False
                            fill_block()
            if distance == 1 and own_way:
                gather_norm()

    for unit in range(2):
        wait_bytes(blob(paired[unit]), pair_recv.at[unit])
    for n, p in enumerate(last_pieces):
        wait_bytes(piece_of(p, ny - 1, nx - 1, 1 - core), both_recv.at[n])
    for kind, halves in enumerate(sent):
        if halves:
            wait_bytes(blob(halves), sent_sem.at[kind])
    for n in range(len(early_pieces)):
        wait_bytes(early.at[n, pl.ds(0, cut)], sent_sem.at[3 + n])
    wait_bytes(peaks.at[0, pl.ds(0, n_shard - 1), :, across_group(0)], peak_send.at[0])
    for g in range(1, len(groups)):
        wait_bytes(chip_peaks.at[reach[g][0], :, :, across_group(g)], peak_send.at[g])

    @pl.when(is_lead)
    def _():
        wait_bytes(norm_all.at[pl.ds(0, n_model - 1)], z_send)
        wait_bytes(blob((n_shard - 1) * math.prod(norm_all.shape) * 2), all_send)

    @pl.when(jnp.logical_not(is_lead))
    def _():
        wait_bytes(norm_mine, mine_send)


def store_kernel(count, parts, *refs):
    pairs = list(zip(refs[:count], refs[count:-1]))
    for n, (src, dst) in enumerate(pairs):
        pieces = parts if src.shape[0] % (parts * 16) == 0 else 1
        size = src.shape[0] // pieces
        for part in range(pieces):
            span = pl.ds(part * size, size)
            pltpu.make_async_copy(src.at[span], dst.at[span], refs[-1].at[n]).start()
    for n, (src, dst) in enumerate(pairs):
        pltpu.make_async_copy(src, dst, refs[-1].at[n]).wait()


def store(arrays, parts):
    hbm = pl.BlockSpec(memory_space=pltpu.HBM)
    return pl.pallas_call(
        functools.partial(store_kernel, len(arrays), parts),
        out_shape=tuple(pltpu.HBM(a.shape, a.dtype) for a in arrays),
        in_specs=[pl.BlockSpec(memory_space=pltpu.VMEM)] * len(arrays),
        out_specs=(hbm,) * len(arrays),
        scratch_shapes=[pltpu.SemaphoreType.DMA((len(arrays),))],
        compiler_params=pltpu.CompilerParams(vmem_limit_bytes=1024 * 1024),
        cost_estimate=pl.CostEstimate(flops=10**9, bytes_accessed=0, transcendentals=0),
    )(*(pltpu.with_memory_space_constraint(a, pltpu.VMEM) for a in arrays))


def patch_kernel(ny, nx, serve, direct, swapped, out, sem):
    me = lax.axis_index("shard")
    core = lax.rem(me, 2)
    chip = me // 2
    missing = lax.rem(chip // nx + 1, ny) * nx + lax.rem(lax.rem(chip, nx) + 1, nx)
    height, width = direct.shape
    span = pl.ds(pl.multiple_of(missing * height, height), height)
    for n, (src, side) in enumerate(((direct, core), (swapped, 1 - core))):
        dst = out.at[span, pl.ds(pl.multiple_of(side * width, width), width)]
        pltpu.make_async_copy(src, dst, sem.at[n]).start()
    for n, src in enumerate((direct, swapped)):
        pltpu.make_async_copy(src, out.at[span, pl.ds(0, width)], sem.at[n]).wait()


def patch(ny, nx, serve, direct, swapped):
    hbm = pl.BlockSpec(memory_space=pltpu.HBM)
    vmem = pl.BlockSpec(memory_space=pltpu.VMEM)
    return pl.pallas_call(
        functools.partial(patch_kernel, ny, nx),
        out_shape=pltpu.HBM(serve.shape, serve.dtype),
        in_specs=[hbm, vmem, vmem],
        out_specs=hbm,
        scratch_shapes=[pltpu.SemaphoreType.DMA((2,))],
        input_output_aliases={0: 0},
        compiler_params=pltpu.CompilerParams(vmem_limit_bytes=1024 * 1024),
    )(serve, *(pltpu.with_memory_space_constraint(a, pltpu.VMEM) for a in (direct, swapped)))


def solution(mesh):
    n_shard, n_model = mesh.shape["shard"], mesh.shape["model"]
    ny, nx = grid_of(n_shard)
    onward_pairs, swap_pairs = [], []
    for chip in range(ny * nx):
        y, x = divmod(chip, nx)
        beside, above = y * nx + (x + 1) % nx, (y + 1) % ny * nx + x
        onward_pairs += [(2 * chip, 2 * beside), (2 * chip + 1, 2 * above + 1)]
        swap_pairs += [(2 * chip, 2 * chip + 1), (2 * chip + 1, 2 * chip)]

    def body(weight_gate, smooth_gate, weight_up, smooth_up, norm_train, norm_step):
        rows, cols = weight_gate.shape
        per = norm_train.shape[0]
        ends = min(nx, ny) > 1 and cols % (8 * LANES) == 0
        pieces = pieces_of(rows, cols, ends)
        reach = cols // LANES // 4 * LANES if ends else LANES
        spans = spans_of(pieces)
        count = len(pieces)
        wide = -(-per // LANES) * LANES
        width = n_shard * n_model * per
        tiles = -(-width // LANES)
        vmem = pl.BlockSpec(memory_space=pltpu.VMEM)
        hbm = pl.BlockSpec(memory_space=pltpu.HBM)
        dma = pltpu.SemaphoreType.DMA
        landed = pl.pallas_call(
            functools.partial(kernel, n_shard, n_model, ny, nx, pieces, spans),
            out_shape=(
                pltpu.VMEM((n_shard * rows, cols), jnp.bfloat16),
                pltpu.VMEM((n_shard * rows, cols), jnp.bfloat16),
                pltpu.VMEM((1, cols), jnp.float32),
                pltpu.VMEM((1, cols), jnp.float32),
                pltpu.VMEM((tiles, LANES), jnp.bfloat16),
                pltpu.VMEM((rows, cols), jnp.float32),
                pltpu.VMEM((rows, cols), jnp.float32),
                pltpu.VMEM((2 * rows, reach), jnp.bfloat16),
            ),
            in_specs=[hbm] * 6,
            out_specs=(vmem,) * 8,
            scratch_shapes=[
                pltpu.VMEM((2, 2, rows, cols), jnp.float32),
                pltpu.VMEM((2, n_shard, 1, cols), jnp.float32),
                pltpu.VMEM((2, ny * nx, 1, cols), jnp.float32),
                pltpu.VMEM((2, rows, LANES), jnp.float32),
                pltpu.VMEM((2, 1, per), jnp.float32),
                pltpu.VMEM((1, wide), jnp.float32),
                pltpu.VMEM((n_model, n_shard, 1, wide), jnp.float32),
                pltpu.VMEM((tiles, LANES), jnp.float32),
                dma((len(spans),)),
                dma((3,)),
                dma((3,)),
                dma((3,)),
                dma((count * (ny * nx - 2),)),
                dma((2,)),
                dma((3,)),
                dma((2,)),
                dma((5,)),
                dma((7,)),
            ],
            compiler_params=pltpu.CompilerParams(
                collective_id=0, has_side_effects=True, vmem_limit_bytes=20 * 1024 * 1024
            ),
        )(
            *(
                pltpu.with_memory_space_constraint(a, pltpu.HBM)
                for a in (weight_gate, smooth_gate, weight_up, smooth_up, norm_train[None], norm_step[None])
            ),
        )
        *landed, whole_up, block = landed
        if ends:
            direct = lax.ppermute(block, "shard", onward_pairs)
        serve_gate, serve_up, factor_gate, factor_up, norm, whole_gate = store(landed, 4)
        if ends:
            direct, whole_up, serve_up = lax.optimization_barrier((direct, whole_up, serve_up))
            swapped = lax.ppermute(direct, "shard", swap_pairs)
        (whole_up,) = store([whole_up], 4)
        if ends:
            serve_up = patch(ny, nx, serve_up, direct, swapped)
        return (
            serve_gate, serve_up, factor_gate.reshape(-1), factor_up.reshape(-1),
            norm.reshape(-1)[:width], whole_gate, whole_up,
        )

    in_specs = (P("shard", "model"),) * 4 + (P(("shard", "model")),) * 2
    out_specs = (
        P(None, "model"),
        P(None, "model"),
        P("model"),
        P("model"),
        P(),
        P("shard", "model"),
        P("shard", "model"),
    )
    return jax.shard_map(body, mesh=mesh, in_specs=in_specs, out_specs=out_specs, check_vma=False)
```

```python
import functools
import math

import jax
import jax.numpy as jnp
from jax import lax
from jax.experimental import pallas as pl
from jax.experimental.pallas import tpu as pltpu
from jax.sharding import PartitionSpec as P

MESH = pl.DeviceIdType.MESH
keep_rate = 0.7
LANES = 128


def grid_of(n_shard):
    chips = n_shard // 2
    nx = math.isqrt(chips)
    while chips % nx:
        nx -= 1
    return chips // nx, nx


def pieces_of(rows, cols, ends):
    tiles = cols // LANES
    cut = rows * 3 // 4 // 16 * 16
    found, tails = [], []
    for unit in range(2):
        at = 0
        queues = []
        for along_x, many in ((True, (tiles + 1) // 2), (False, tiles // 2)):
            if many < 4 or not ends:
                queues.append([(along_x, 1, None)] * many)
            elif unit == 0:
                queues.append([(along_x, 2, None), (along_x, 1, "early"), (along_x, many - 3, None)])
            else:
                near = many // 2
                queues.append([(along_x, near, "near"), (along_x, many - near - 1, None), (along_x, 1, "loose")])
        for n in range(max(len(q) for q in queues)):
            for queue in queues:
                if n < len(queue):
                    along_x, width, kind = queue[n]
                    here = (unit, at * LANES, width * LANES)
                    at += width
                    if kind == "early":
                        found.append(here + (0, cut, along_x, kind))
                        tails.append(here + (cut, rows - cut, along_x, None))
                    else:
                        found.append(here + (0, rows, along_x, kind))
        found += tails
        tails = []
    return found


def is_early_landing(piece, dy, dx):
    return piece[6] == "early" and (dy, dx) == ((0, 1) if piece[5] else (1, 0))


def landings_of(pieces, ny, nx):
    found = {}
    far = (ny - 1, nx - 1)
    for p, piece in enumerate(pieces):
        unit, along_x, kind = piece[0], piece[5], piece[6]
        for dy in range(ny):
            for dx in range(nx):
                if (dy, dx) == (0, 0) or (kind == "near" and (dy, dx) == far):
                    continue
                key = (unit, along_x, dy, dx)
                if (dy, dx) == ((1, 0) if along_x else (0, 1)):
                    key = unit
                elif is_early_landing(piece, dy, dx) or (unit and (dy, dx) == far):
                    key = (p, dy, dx)
                found.setdefault(key, []).append((p, dy, dx))
    return found


def spans_of(pieces):
    spans = []
    for unit, at, width, top, _, _, _ in pieces:
        if top:
            continue
        if spans and spans[-1][0] == unit and spans[-1][2] == width and width <= 2 * LANES:
            spans[-1] = (unit, spans[-1][1], spans[-1][2] + width)
        else:
            spans.append((unit, at, width))
    return spans


def kernel(
    n_shard, n_model, ny, nx, pieces, spans,
    weight_gate, smooth_gate, weight_up, smooth_up, norm_train, norm_step,
    serve_gate, serve_up, factor_gate, factor_up, norm_out, whole_gate, whole_up, block, loose,
    inputs, peaks, chip_peaks, early, norm_in, norm_mine, norm_all, norm_rows,
    load_sem, peak_send, peak_recv, couple_recv, ring_recv, pair_recv, sent_sem, small_sem,
):
    me = lax.axis_index("shard")
    col = lax.axis_index("model")
    core = lax.rem(me, 2)
    chip = me // 2
    xpos, ypos = lax.rem(chip, nx), chip // nx
    x_next = (ypos * nx + lax.rem(xpos + 1, nx)) * 2 + core
    y_next = (lax.rem(ypos + 1, ny) * nx + xpos) * 2 + core
    pair = chip * 2 + (1 - core)
    rows, cols = whole_gate.shape
    serves, wholes, factors = (serve_gate, serve_up), (whole_gate, whole_up), (factor_gate, factor_up)
    order = range(len(pieces))
    early_pieces = [p for p in order if pieces[p][6] == "early"]
    loose_pieces = [p for p in order if pieces[p][6] == "loose"]
    near_pieces = [p for p in order if pieces[p][6] == "near"]
    far = (ny - 1, nx - 1)
    chips = ny * nx
    lead = 1
    is_lead = me == lead
    per = norm_train.shape[1]
    norm_load, mine_send, mine_recv, z_send, z_recv, all_send, all_recv = [small_sem.at[i] for i in range(7)]

    def across(p):
        return pl.ds(pieces[p][1], pieces[p][2])

    def wait_bytes(ref, sem):
        pltpu.make_async_copy(ref, ref, sem).wait()

    def blob(halves):
        wide = next(
            w for w in range(LANES, cols + 1, LANES) if halves % (8 * w) == 0 and halves // w <= n_shard * rows
        )
        return serve_gate.at[pl.ds(0, halves // wide), pl.ds(0, wide)]

    groups = [[], [], []]
    for p in order:
        unit, at = pieces[p][:2]
        groups[2 if unit else int(at >= sum(spans[0][1:]))].append(p)
    groups = [g for g in groups if g]
    reach = [
        (pieces[g[0]][0], pieces[g[0]][1], sum(pieces[p][2] for p in g if pieces[p][3] == 0)) for g in groups
    ]

    barrier = pltpu.get_barrier_semaphore()
    for d in range(1, n_shard):
        pl.semaphore_signal(barrier, inc=1, device_id=(lax.rem(me + d, n_shard), col), device_id_type=MESH)

    @pl.when(is_lead)
    def _():
        for d in range(1, n_model):
            pl.semaphore_signal(barrier, inc=1, device_id=(me, lax.rem(col + d, n_model)), device_id_type=MESH)

    sources = ((weight_gate, smooth_gate), (weight_up, smooth_up))
    for n, (unit, at, width) in enumerate(spans):
        for which in range(2):
            pltpu.make_async_copy(
                sources[unit][which].at[:, pl.ds(at, width)], inputs.at[which, unit, :, pl.ds(at, width)], load_sem.at[n]
            ).start()
    for i, src in enumerate((norm_train, norm_step)):
        pltpu.make_async_copy(src, norm_in.at[i], norm_load).start()

    def average(n):
        unit, first, width = spans[n]
        here = pl.ds(first, width)
        wait_bytes(inputs.at[:, unit, :, here], load_sem.at[n])

        def step(i, top):
            rows_now = pl.ds(pl.multiple_of(i * 8, 8), 8)
            value = keep_rate * inputs[1, unit, rows_now, here] + (1.0 - keep_rate) * inputs[0, unit, rows_now, here]
            wholes[unit][rows_now, here] = value
            return jnp.maximum(top, jnp.abs(value))

        top = lax.fori_loop(0, rows // 8, step, jnp.zeros((8, width), jnp.float32), unroll=4)
        peaks[unit, me, :, here] = jnp.max(top, axis=0, keepdims=True)

    def start(src, dst, device, send_sem, recv_sem):
        pltpu.make_async_remote_copy(
            src_ref=src, dst_ref=dst, send_sem=send_sem, recv_sem=recv_sem,
            device_id=device, device_id_type=MESH,
        ).start()

    def across_group(g):
        return pl.ds(reach[g][1], reach[g][2])

    def send_peaks(g):
        ref = peaks.at[reach[g][0], me, :, across_group(g)]
        if g == 0:
            for d in range(1, n_shard):
                start(ref, ref, (lax.rem(me + d, n_shard), col), peak_send.at[g], peak_recv.at[g])
        else:
            start(ref, ref, (pair, col), peak_send.at[g], couple_recv.at[g])

    def combine_peaks(g):
        unit, here = reach[g][0], across_group(g)
        wait_bytes(peaks.at[unit, 0, :, here], couple_recv.at[g])
        chip_peaks[unit, chip, :, here] = jnp.maximum(peaks[unit, me, :, here], peaks[unit, pair, :, here])

    def spread_peaks(g):
        ref = chip_peaks.at[reach[g][0], chip, :, across_group(g)]
        for d in range(1, chips):
            start(ref, ref, (lax.rem(me + 2 * d, n_shard), col), peak_send.at[g], peak_recv.at[g])

    def piece_of(p, dy, dx, side):
        owner = (lax.rem(ypos - dy + ny, ny) * nx + lax.rem(xpos - dx + nx, nx)) * 2 + side
        unit, _, _, top, height = pieces[p][:5]
        return serves[unit].at[pl.ds(pl.multiple_of(owner * rows + top, 16), height), across(p)]

    def along_x_first(p):
        return pieces[p][5]

    def landed_early(p, dy, dx):
        return is_early_landing(pieces[p], dy, dx)

    gathers = landings_of(pieces, ny, nx)
    keys = list(gathers)

    def key_of(p, dy, dx):
        return next(key for key in keys if (p, dy, dx) in gathers[key])

    def landing(p, dy, dx):
        return ring_recv.at[keys.index(key_of(p, dy, dx))]

    sent = [0, 0, 0]
    paired = [0, 0, 0]

    def send(p, spot, device, sem, dst=None):
        ref = piece_of(p, *spot, core)
        kind = 2 if p in early_pieces else pieces[p][0]
        sent[kind] += pieces[p][2] * pieces[p][4]
        start(ref, ref if dst is None else dst, (device, col), sent_sem.at[kind], sem)

    def loose_ref(p):
        return loose.at[:, pl.ds(loose_pieces.index(p) * LANES, LANES)]

    def onward(p, spot, device, there):
        if p in near_pieces and there == far:
            return
        send(p, spot, device, landing(p, *there), loose_ref(p) if p in loose_pieces and there == far else None)

    def to_x(p, dy, dx):
        if dx < nx - 1 and (dy == 0 or not along_x_first(p)):
            onward(p, (dy, dx), x_next, (dy, dx + 1))

    def to_y(p, dy, dx):
        if dy < ny - 1 and (dx == 0 or along_x_first(p)):
            onward(p, (dy, dx), y_next, (dy + 1, dx))

    def to_pair(p, dy, dx):
        if not (p in loose_pieces and (dy, dx) == far):
            kind = 2 if p in near_pieces else pieces[p][0]
            paired[kind] += pieces[p][2] * pieces[p][4]
            send(p, (dy, dx), pair, pair_recv.at[kind])

    def first_way(p):
        (to_x if along_x_first(p) else to_y)(p, 0, 0)

    def second_way(p):
        (to_y if along_x_first(p) else to_x)(p, 0, 0)

    cut = pieces[early_pieces[0]][4] if early_pieces else 0
    chunks = 3 if cut % 24 == 0 else 1

    def send_early(chunk):
        span = pl.ds(chunk * (cut // chunks), cut // chunks)
        for n, p in enumerate(early_pieces):
            device, spot = (x_next, (0, 1)) if along_x_first(p) else (y_next, (1, 0))
            start(
                wholes[pieces[p][0]].at[span, across(p)], early.at[n, span], (device, col),
                sent_sem.at[3 + n], landing(p, *spot),
            )

    def find_factor(g):
        unit, here = reach[g][0], across_group(g)
        table, many = (peaks, n_shard) if g == 0 else (chip_peaks, chips)
        if many > 1:
            wait_bytes(table.at[unit, pl.ds(0, many - 1), :, here], peak_recv.at[g])
        factor = table[unit, 0, :, here]
        for d in range(1, many):
            factor = jnp.maximum(factor, table[unit, d, :, here])
        factors[unit][:, here] = factor

    def narrow(p, owner, read):
        unit, _, _, top, height = pieces[p][:5]

        def step(i, carry):
            at = top + i * 16
            value = read(pl.ds(pl.multiple_of(at, 16), 16)) / factors[unit][:, across(p)]
            serves[unit][pl.ds(pl.multiple_of(owner * rows + at, 16), 16), across(p)] = value.astype(jnp.bfloat16)
            return carry

        lax.fori_loop(0, height // 16, step, 0, unroll=2)

    def narrow_own(p):
        narrow(p, me, lambda span: wholes[pieces[p][0]][span, across(p)])

    here_now = set()

    def arrived(p, dy, dx):
        key = key_of(p, dy, dx)
        if key not in here_now:
            here_now.add(key)
            if landed_early(p, dy, dx):
                wait_bytes(early.at[early_pieces.index(p), pl.ds(0, cut)], landing(p, dy, dx))
            else:
                wait_bytes(blob(sum(pieces[q][2] * pieces[q][4] for q, _, _ in gathers[key])), landing(p, dy, dx))
        if landed_early(p, dy, dx):
            n = early_pieces.index(p)
            owner = (lax.rem(ypos - dy + ny, ny) * nx + lax.rem(xpos - dx + nx, nx)) * 2 + core
            narrow(p, owner, lambda span: early[n, span])

    def norm_sum():
        wait_bytes(norm_in, norm_load)
        norm_mine[...] = jnp.zeros(norm_mine.shape, jnp.float32)
        norm_mine[:, 0:per] = norm_in[0] + norm_in[1]

    def norm_to_lead():
        @pl.when(jnp.logical_not(is_lead))
        def _():
            start(norm_mine, norm_all.at[col, me], (lead, col), mine_send, mine_recv)

    def norm_spread():
        @pl.when(is_lead)
        def _():
            norm_all[col, me] = norm_mine[...]
            wait_bytes(norm_all.at[0, pl.ds(0, n_shard - 1)], mine_recv)
            for d in range(1, n_model):
                start(norm_all.at[col], norm_all.at[col], (me, lax.rem(col + d, n_model)), z_send, z_recv)
            wait_bytes(norm_all.at[pl.ds(0, n_model - 1)], z_recv)
            for d in range(1, n_shard):
                start(norm_all, norm_all, (lax.rem(me + d, n_shard), col), all_send, all_recv)

    average(0)

    @pl.when(is_lead)
    def _():
        pl.semaphore_wait(barrier, n_shard + n_model - 2)

    @pl.when(jnp.logical_not(is_lead))
    def _():
        pl.semaphore_wait(barrier, n_shard - 1)

    ready, chunk = 0, 0
    for n, (unit, at, width) in enumerate(spans):
        final = n == len(spans) - 1
        if final and ready > 1:
            combine_peaks(1)
        if n:
            average(n)
        if (unit, at + width) == (reach[ready][0], sum(reach[ready][1:])):
            send_peaks(ready)
            ready += 1
        if n and chunk < chunks and early_pieces:
            send_early(chunk)
            chunk += 1
    if len(groups) > 1:
        spread_peaks(1)

    for g, group in enumerate(groups):
        find_factor(g)
        before = None
        for p in [p for p in group if p not in early_pieces] + [p for p in group if p in early_pieces]:
            narrow_own(p)
            if before is not None:
                first_way(before)
            before = None if p in early_pieces else p
        if g == 0:
            norm_sum()
        if g == len(groups) - 1:
            for p in groups[0]:
                to_pair(p, 0, 0)
        if before is not None:
            first_way(before)
        if g == 0:
            for later in range(2, len(groups)):
                combine_peaks(later)
            norm_to_lead()
            for later in range(2, len(groups)):
                spread_peaks(later)
    norm_spread()
    for p in order:
        if p not in early_pieces:
            second_way(p)
    for p in early_pieces:
        second_way(p)
    for group in groups[1:]:
        for p in group:
            to_pair(p, 0, 0)

    def gather_norm():
        @pl.when(jnp.logical_not(is_lead))
        def _():
            wait_bytes(norm_all, all_recv)

        lane = lax.broadcasted_iota(jnp.int32, (8, LANES), 1)
        tiles = [jnp.zeros((8, LANES), jnp.float32) for _ in range(norm_out.shape[0])]
        for s in range(n_shard):
            for c in range(n_model):
                for at in range(0, per, LANES):
                    size = min(LANES, per - at)
                    tile, shift = divmod((s * n_model + c) * per + at, LANES)
                    row = jnp.broadcast_to(norm_all[c, s, :, at:at + LANES], (8, LANES))
                    if shift:
                        row = pltpu.roll(row, shift, 1)
                    tiles[tile] = jnp.where((lane >= shift) & (lane < shift + size), row, tiles[tile])
                    if shift + size > LANES:
                        tiles[tile + 1] = jnp.where(lane < shift + size - LANES, row, tiles[tile + 1])
        for t, tile in enumerate(tiles):
            norm_rows[t:t + 1] = tile[0:1]
        norm_out[...] = norm_rows[...].astype(jnp.bfloat16)

    def fill_block():
        wait_bytes(blob(paired[2]), pair_recv.at[2])
        chosen = lax.rem(ypos + 1 + core, ny) * nx + lax.rem(xpos + 2 - core, nx)
        base = 2 * rows * chosen
        width = block.shape[1]
        for c in range(2):
            @pl.when(core == c)
            def _():
                def step(i, carry):
                    block[pl.ds(pl.multiple_of(i * 16, 16), 16)] = serve_up[
                        pl.ds(pl.multiple_of(base + i * 16, 16), 16), c * width:(c + 1) * width
                    ]
                    return carry

                lax.fori_loop(0, 2 * rows // 16, step, 0, unroll=4)

    block_due = bool(near_pieces)
    for distance in range(1, ny + nx - 1):
        for own_way in (True, False):
            for p in order:
                for dy in range(ny):
                    dx = distance - dy
                    straight = (dy if along_x_first(p) else dx) == 0
                    if p in near_pieces and (dy, dx) == far:
                        continue
                    if 0 <= dx < nx and straight == own_way:
                        arrived(p, dy, dx)
                        to_x(p, dy, dx)
                        to_y(p, dy, dx)
                        to_pair(p, dy, dx)
                        if block_due and (dy, dx) == far:
                            block_due = False
                            fill_block()
            if distance == 1 and own_way:
                gather_norm()

    for unit in range(2):
        wait_bytes(blob(paired[unit]), pair_recv.at[unit])
    for kind, halves in enumerate(sent):
        if halves:
            wait_bytes(blob(halves), sent_sem.at[kind])
    for n in range(len(early_pieces)):
        wait_bytes(early.at[n, pl.ds(0, cut)], sent_sem.at[3 + n])
    wait_bytes(peaks.at[0, pl.ds(0, n_shard - 1), :, across_group(0)], peak_send.at[0])
    for g in range(1, len(groups)):
        wait_bytes(chip_peaks.at[reach[g][0], :, :, across_group(g)], peak_send.at[g])

    @pl.when(is_lead)
    def _():
        wait_bytes(norm_all.at[pl.ds(0, n_model - 1)], z_send)
        wait_bytes(blob((n_shard - 1) * math.prod(norm_all.shape) * 2), all_send)

    @pl.when(jnp.logical_not(is_lead))
    def _():
        wait_bytes(norm_mine, mine_send)


def store_kernel(count, parts, *refs):
    pairs = list(zip(refs[:count], refs[count:-1]))
    for n, (src, dst) in enumerate(pairs):
        pieces = parts if src.shape[0] % (parts * 16) == 0 else 1
        size = src.shape[0] // pieces
        for part in range(pieces):
            span = pl.ds(part * size, size)
            pltpu.make_async_copy(src.at[span], dst.at[span], refs[-1].at[n]).start()
    for n, (src, dst) in enumerate(pairs):
        pltpu.make_async_copy(src, dst, refs[-1].at[n]).wait()


def store(arrays, parts):
    hbm = pl.BlockSpec(memory_space=pltpu.HBM)
    return pl.pallas_call(
        functools.partial(store_kernel, len(arrays), parts),
        out_shape=tuple(pltpu.HBM(a.shape, a.dtype) for a in arrays),
        in_specs=[pl.BlockSpec(memory_space=pltpu.VMEM)] * len(arrays),
        out_specs=(hbm,) * len(arrays),
        scratch_shapes=[pltpu.SemaphoreType.DMA((len(arrays),))],
        compiler_params=pltpu.CompilerParams(vmem_limit_bytes=1024 * 1024),
        cost_estimate=pl.CostEstimate(flops=10**9, bytes_accessed=0, transcendentals=0),
    )(*(pltpu.with_memory_space_constraint(a, pltpu.VMEM) for a in arrays))


def patch_kernel(ny, nx, kinds, *refs):
    me = lax.axis_index("shard")
    core = lax.rem(me, 2)
    chip = me // 2
    missing = lax.rem(chip // nx + 1, ny) * nx + lax.rem(lax.rem(chip, nx) + 1, nx)
    blocks, rest, sem = refs[1:1 + len(kinds)], refs[1 + len(kinds):-1], refs[-1]
    extra, (out, *stored) = rest[:len(rest) // 2], rest[len(rest) // 2:]
    waits = []
    for n, (kind, src) in enumerate(zip(kinds, blocks)):
        height, width = src.shape
        if kind in ("direct", "swapped"):
            row = missing * height
            side = core if kind == "direct" else 1 - core
            across = pl.ds(pl.multiple_of(side * width, width), width)
        else:
            row = (2 * missing + (core if kind == "loose" else 1 - core)) * height
            across = pl.ds(out.shape[1] - width, width)
        span = pl.ds(pl.multiple_of(row, 16), height)
        waits.append(pltpu.make_async_copy(src, out.at[span, across], sem.at[n]))
        waits[-1].start()
    for n, (src, dst) in enumerate(zip(extra, stored)):
        waits.append(pltpu.make_async_copy(src, dst, sem.at[len(kinds) + n]))
        waits[-1].start()
    for copy in waits:
        copy.wait()


def patch(ny, nx, serve, blocks, extra=()):
    hbm = pl.BlockSpec(memory_space=pltpu.HBM)
    vmem = pl.BlockSpec(memory_space=pltpu.VMEM)
    held = (*blocks.values(), *extra)
    return pl.pallas_call(
        functools.partial(patch_kernel, ny, nx, tuple(blocks)),
        out_shape=tuple(pltpu.HBM(a.shape, a.dtype) for a in (serve, *extra)),
        in_specs=[hbm] + [vmem] * len(held),
        out_specs=(hbm,) * (1 + len(extra)),
        scratch_shapes=[pltpu.SemaphoreType.DMA((len(held),))],
        input_output_aliases={0: 0},
        compiler_params=pltpu.CompilerParams(vmem_limit_bytes=1024 * 1024),
        cost_estimate=pl.CostEstimate(flops=10**9, bytes_accessed=0, transcendentals=0),
    )(serve, *(pltpu.with_memory_space_constraint(a, pltpu.VMEM) for a in held))


def solution(mesh):
    n_shard, n_model = mesh.shape["shard"], mesh.shape["model"]
    ny, nx = grid_of(n_shard)
    onward_pairs, swap_pairs = [], []
    for chip in range(ny * nx):
        y, x = divmod(chip, nx)
        beside, above = y * nx + (x + 1) % nx, (y + 1) % ny * nx + x
        onward_pairs += [(2 * chip, 2 * beside), (2 * chip + 1, 2 * above + 1)]
        swap_pairs += [(2 * chip, 2 * chip + 1), (2 * chip + 1, 2 * chip)]

    def body(weight_gate, smooth_gate, weight_up, smooth_up, norm_train, norm_step):
        rows, cols = weight_gate.shape
        per = norm_train.shape[0]
        ends = min(nx, ny) > 1 and cols % (8 * LANES) == 0
        pieces = pieces_of(rows, cols, ends)
        reach = cols // LANES // 4 * LANES if ends else LANES
        spans = spans_of(pieces)
        count = len(pieces)
        wide = -(-per // LANES) * LANES
        width = n_shard * n_model * per
        tiles = -(-width // LANES)
        vmem = pl.BlockSpec(memory_space=pltpu.VMEM)
        hbm = pl.BlockSpec(memory_space=pltpu.HBM)
        dma = pltpu.SemaphoreType.DMA
        landed = pl.pallas_call(
            functools.partial(kernel, n_shard, n_model, ny, nx, pieces, spans),
            out_shape=(
                pltpu.VMEM((n_shard * rows, cols), jnp.bfloat16),
                pltpu.VMEM((n_shard * rows, cols), jnp.bfloat16),
                pltpu.VMEM((1, cols), jnp.float32),
                pltpu.VMEM((1, cols), jnp.float32),
                pltpu.VMEM((tiles, LANES), jnp.bfloat16),
                pltpu.VMEM((rows, cols), jnp.float32),
                pltpu.VMEM((rows, cols), jnp.float32),
                pltpu.VMEM((2 * rows, reach), jnp.bfloat16),
                pltpu.VMEM((rows, 2 * LANES), jnp.bfloat16),
            ),
            in_specs=[hbm] * 6,
            out_specs=(vmem,) * 9,
            scratch_shapes=[
                pltpu.VMEM((2, 2, rows, cols), jnp.float32),
                pltpu.VMEM((2, n_shard, 1, cols), jnp.float32),
                pltpu.VMEM((2, ny * nx, 1, cols), jnp.float32),
                pltpu.VMEM((2, rows, LANES), jnp.float32),
                pltpu.VMEM((2, 1, per), jnp.float32),
                pltpu.VMEM((1, wide), jnp.float32),
                pltpu.VMEM((n_model, n_shard, 1, wide), jnp.float32),
                pltpu.VMEM((tiles, LANES), jnp.float32),
                dma((len(spans),)),
                dma((3,)),
                dma((3,)),
                dma((3,)),
                dma((len(landings_of(pieces, ny, nx)),)),
                dma((3,)),
                dma((5,)),
                dma((7,)),
            ],
            compiler_params=pltpu.CompilerParams(
                collective_id=0, has_side_effects=True, vmem_limit_bytes=20 * 1024 * 1024
            ),
        )(
            *(
                pltpu.with_memory_space_constraint(a, pltpu.HBM)
                for a in (weight_gate, smooth_gate, weight_up, smooth_up, norm_train[None], norm_step[None])
            ),
        )
        *landed, whole_up, block, loose = landed
        if ends:
            direct = lax.ppermute(block, "shard", onward_pairs)
            paired = lax.ppermute(loose, "shard", swap_pairs)
        serve_gate, serve_up, factor_gate, factor_up, norm, whole_gate = store(landed, 4)
        if ends:
            direct, paired, loose, whole_up, serve_up = lax.optimization_barrier(
                (direct, paired, loose, whole_up, serve_up)
            )
            swapped = lax.ppermute(direct, "shard", swap_pairs)
            first = {"direct": direct, "loose": loose, "paired": paired}
            serve_up, whole_up = patch(ny, nx, serve_up, first, (whole_up,))
            (serve_up,) = patch(ny, nx, serve_up, {"swapped": swapped})
        else:
            (whole_up,) = store([whole_up], 4)
        return (
            serve_gate, serve_up, factor_gate.reshape(-1), factor_up.reshape(-1),
            norm.reshape(-1)[:width], whole_gate, whole_up,
        )

    in_specs = (P("shard", "model"),) * 4 + (P(("shard", "model")),) * 2
    out_specs = (
        P(None, "model"),
        P(None, "model"),
        P("model"),
        P("model"),
        P(),
        P("shard", "model"),
        P("shard", "model"),
    )
    return jax.shard_map(body, mesh=mesh, in_specs=in_specs, out_specs=out_specs, check_vma=False)
```

```python
import functools
import math

import jax
import jax.numpy as jnp
from jax import lax
from jax.experimental import pallas as pl
from jax.experimental.pallas import tpu as pltpu
from jax.sharding import PartitionSpec as P

MESH = pl.DeviceIdType.MESH
keep_rate = 0.7
LANES = 128


def grid_of(n_shard):
    chips = n_shard // 2
    nx = math.isqrt(chips)
    while chips % nx:
        nx -= 1
    return chips // nx, nx


def pieces_of(rows, cols, ends):
    tiles = cols // LANES
    cut = rows * 3 // 4 // 16 * 16
    found, tails = [], []
    for unit in range(2):
        at = 0
        queues = []
        for along_x, many in ((True, (tiles + 1) // 2), (False, tiles // 2)):
            if many < 4 or not ends:
                queues.append([(along_x, 1, None)] * many)
            elif unit == 0:
                queues.append([(along_x, 2, None), (along_x, 1, "early"), (along_x, many - 3, None)])
            else:
                near = many // 2
                queues.append([(along_x, near, "near"), (along_x, many - near - 1, None), (along_x, 1, "loose")])
        for n in range(max(len(q) for q in queues)):
            for queue in queues:
                if n < len(queue):
                    along_x, width, kind = queue[n]
                    here = (unit, at * LANES, width * LANES)
                    at += width
                    if kind == "early":
                        found.append(here + (0, cut, along_x, kind))
                        tails.append(here + (cut, rows - cut, along_x, None))
                    else:
                        found.append(here + (0, rows, along_x, kind))
        found += tails
        tails = []
    return found


def is_early_landing(piece, dy, dx):
    return piece[6] == "early" and (dy, dx) == ((0, 1) if piece[5] else (1, 0))


def landings_of(pieces, ny, nx):
    found = {}
    far = (ny - 1, nx - 1)
    for p, piece in enumerate(pieces):
        unit, along_x, kind = piece[0], piece[5], piece[6]
        for dy in range(ny):
            for dx in range(nx):
                if (dy, dx) == (0, 0) or (kind == "near" and (dy, dx) == far):
                    continue
                key = (unit, along_x, dy, dx)
                if (dy, dx) == ((1, 0) if along_x else (0, 1)):
                    key = unit
                elif is_early_landing(piece, dy, dx) or (unit and (dy, dx) == far):
                    key = (p, dy, dx)
                found.setdefault(key, []).append((p, dy, dx))
    return found


def spans_of(pieces):
    spans = []
    for unit, at, width, top, _, _, _ in pieces:
        if top:
            continue
        if spans and spans[-1][0] == unit and spans[-1][2] == width and width <= 2 * LANES:
            spans[-1] = (unit, spans[-1][1], spans[-1][2] + width)
        else:
            spans.append((unit, at, width))
    return spans


def kernel(
    n_shard, n_model, ny, nx, pieces, spans,
    weight_gate, smooth_gate, weight_up, smooth_up, norm_train, norm_step,
    serve_gate, serve_up, factor_gate, factor_up, norm_out, whole_gate, whole_up, block, loose,
    inputs, peaks, chip_peaks, early, norm_in, norm_mine, norm_all, norm_rows,
    load_sem, peak_send, peak_recv, couple_recv, ring_recv, pair_recv, sent_sem, small_sem,
):
    me = lax.axis_index("shard")
    col = lax.axis_index("model")
    core = lax.rem(me, 2)
    chip = me // 2
    xpos, ypos = lax.rem(chip, nx), chip // nx
    x_next = (ypos * nx + lax.rem(xpos + 1, nx)) * 2 + core
    y_next = (lax.rem(ypos + 1, ny) * nx + xpos) * 2 + core
    pair = chip * 2 + (1 - core)
    rows, cols = whole_gate.shape
    serves, wholes, factors = (serve_gate, serve_up), (whole_gate, whole_up), (factor_gate, factor_up)
    order = range(len(pieces))
    early_pieces = [p for p in order if pieces[p][6] == "early"]
    loose_pieces = [p for p in order if pieces[p][6] == "loose"]
    near_pieces = [p for p in order if pieces[p][6] == "near"]
    far = (ny - 1, nx - 1)
    chips = ny * nx
    lead = 1
    is_lead = me == lead
    per = norm_train.shape[1]
    norm_load, mine_send, mine_recv, z_send, z_recv, all_send, all_recv = [small_sem.at[i] for i in range(7)]

    def across(p):
        return pl.ds(pieces[p][1], pieces[p][2])

    def wait_bytes(ref, sem):
        pltpu.make_async_copy(ref, ref, sem).wait()

    def blob(halves):
        wide = next(
            w for w in range(LANES, cols + 1, LANES) if halves % (8 * w) == 0 and halves // w <= n_shard * rows
        )
        return serve_gate.at[pl.ds(0, halves // wide), pl.ds(0, wide)]

    groups = [[], [], []]
    for p in order:
        unit, at = pieces[p][:2]
        groups[2 if unit else int(at >= sum(spans[0][1:]))].append(p)
    groups = [g for g in groups if g]
    reach = [
        (pieces[g[0]][0], pieces[g[0]][1], sum(pieces[p][2] for p in g if pieces[p][3] == 0)) for g in groups
    ]

    barrier = pltpu.get_barrier_semaphore()
    for d in range(1, n_shard):
        pl.semaphore_signal(barrier, inc=1, device_id=(lax.rem(me + d, n_shard), col), device_id_type=MESH)

    @pl.when(is_lead)
    def _():
        for d in range(1, n_model):
            pl.semaphore_signal(barrier, inc=1, device_id=(me, lax.rem(col + d, n_model)), device_id_type=MESH)

    sources = ((weight_gate, smooth_gate), (weight_up, smooth_up))
    for n, (unit, at, width) in enumerate(spans):
        for which in range(2):
            pltpu.make_async_copy(
                sources[unit][which].at[:, pl.ds(at, width)], inputs.at[which, unit, :, pl.ds(at, width)], load_sem.at[n]
            ).start()
    for i, src in enumerate((norm_train, norm_step)):
        pltpu.make_async_copy(src, norm_in.at[i], norm_load).start()

    def average(n):
        unit, first, width = spans[n]
        here = pl.ds(first, width)
        wait_bytes(inputs.at[:, unit, :, here], load_sem.at[n])

        def step(i, top):
            rows_now = pl.ds(pl.multiple_of(i * 8, 8), 8)
            value = keep_rate * inputs[1, unit, rows_now, here] + (1.0 - keep_rate) * inputs[0, unit, rows_now, here]
            wholes[unit][rows_now, here] = value
            return jnp.maximum(top, jnp.abs(value))

        top = lax.fori_loop(0, rows // 8, step, jnp.zeros((8, width), jnp.float32), unroll=4)
        peaks[unit, me, :, here] = jnp.max(top, axis=0, keepdims=True)

    def start(src, dst, device, send_sem, recv_sem):
        pltpu.make_async_remote_copy(
            src_ref=src, dst_ref=dst, send_sem=send_sem, recv_sem=recv_sem,
            device_id=device, device_id_type=MESH,
        ).start()

    def across_group(g):
        return pl.ds(reach[g][1], reach[g][2])

    def send_peaks(g):
        ref = peaks.at[reach[g][0], me, :, across_group(g)]
        if g == 0:
            for d in range(1, n_shard):
                start(ref, ref, (lax.rem(me + d, n_shard), col), peak_send.at[g], peak_recv.at[g])
        else:
            start(ref, ref, (pair, col), peak_send.at[g], couple_recv.at[g])

    def combine_peaks(g):
        unit, here = reach[g][0], across_group(g)
        wait_bytes(peaks.at[unit, 0, :, here], couple_recv.at[g])
        chip_peaks[unit, chip, :, here] = jnp.maximum(peaks[unit, me, :, here], peaks[unit, pair, :, here])

    def spread_peaks(g):
        ref = chip_peaks.at[reach[g][0], chip, :, across_group(g)]
        for d in range(1, chips):
            start(ref, ref, (lax.rem(me + 2 * d, n_shard), col), peak_send.at[g], peak_recv.at[g])

    def piece_of(p, dy, dx, side):
        owner = (lax.rem(ypos - dy + ny, ny) * nx + lax.rem(xpos - dx + nx, nx)) * 2 + side
        unit, _, _, top, height = pieces[p][:5]
        return serves[unit].at[pl.ds(pl.multiple_of(owner * rows + top, 16), height), across(p)]

    def along_x_first(p):
        return pieces[p][5]

    def landed_early(p, dy, dx):
        return is_early_landing(pieces[p], dy, dx)

    gathers = landings_of(pieces, ny, nx)
    keys = list(gathers)

    def key_of(p, dy, dx):
        return next(key for key in keys if (p, dy, dx) in gathers[key])

    def landing(p, dy, dx):
        return ring_recv.at[keys.index(key_of(p, dy, dx))]

    sent = [0, 0, 0]
    paired = [0, 0, 0]

    def send(p, spot, device, sem, dst=None):
        ref = piece_of(p, *spot, core)
        kind = 2 if p in early_pieces else pieces[p][0]
        sent[kind] += pieces[p][2] * pieces[p][4]
        start(ref, ref if dst is None else dst, (device, col), sent_sem.at[kind], sem)

    def loose_ref(p):
        return loose.at[:, pl.ds(loose_pieces.index(p) * LANES, LANES)]

    def onward(p, spot, device, there):
        if p in near_pieces and there == far:
            return
        send(p, spot, device, landing(p, *there), loose_ref(p) if p in loose_pieces and there == far else None)

    def to_x(p, dy, dx):
        if dx < nx - 1 and (dy == 0 or not along_x_first(p)):
            onward(p, (dy, dx), x_next, (dy, dx + 1))

    def to_y(p, dy, dx):
        if dy < ny - 1 and (dx == 0 or along_x_first(p)):
            onward(p, (dy, dx), y_next, (dy + 1, dx))

    def to_pair(p, dy, dx):
        if not (p in loose_pieces and (dy, dx) == far):
            kind = 2 if p in near_pieces else pieces[p][0]
            paired[kind] += pieces[p][2] * pieces[p][4]
            send(p, (dy, dx), pair, pair_recv.at[kind])

    def first_way(p):
        (to_x if along_x_first(p) else to_y)(p, 0, 0)

    def second_way(p):
        (to_y if along_x_first(p) else to_x)(p, 0, 0)

    cut = pieces[early_pieces[0]][4] if early_pieces else 0
    chunks = 3 if cut % 24 == 0 else 1

    def send_early(chunk):
        span = pl.ds(chunk * (cut // chunks), cut // chunks)
        for n, p in enumerate(early_pieces):
            device, spot = (x_next, (0, 1)) if along_x_first(p) else (y_next, (1, 0))
            start(
                wholes[pieces[p][0]].at[span, across(p)], early.at[n, span], (device, col),
                sent_sem.at[3 + n], landing(p, *spot),
            )

    def find_factor(g):
        unit, here = reach[g][0], across_group(g)
        table, many = (peaks, n_shard) if g == 0 else (chip_peaks, chips)
        if many > 1:
            wait_bytes(table.at[unit, pl.ds(0, many - 1), :, here], peak_recv.at[g])
        factor = table[unit, 0, :, here]
        for d in range(1, many):
            factor = jnp.maximum(factor, table[unit, d, :, here])
        factors[unit][:, here] = factor

    def narrow(p, owner, read):
        unit, _, _, top, height = pieces[p][:5]

        def step(i, carry):
            at = top + i * 16
            value = read(pl.ds(pl.multiple_of(at, 16), 16)) / factors[unit][:, across(p)]
            serves[unit][pl.ds(pl.multiple_of(owner * rows + at, 16), 16), across(p)] = value.astype(jnp.bfloat16)
            return carry

        lax.fori_loop(0, height // 16, step, 0, unroll=2)

    def narrow_own(p):
        narrow(p, me, lambda span: wholes[pieces[p][0]][span, across(p)])

    here_now = set()

    def arrived(p, dy, dx):
        key = key_of(p, dy, dx)
        if key not in here_now:
            here_now.add(key)
            if landed_early(p, dy, dx):
                wait_bytes(early.at[early_pieces.index(p), pl.ds(0, cut)], landing(p, dy, dx))
            else:
                wait_bytes(blob(sum(pieces[q][2] * pieces[q][4] for q, _, _ in gathers[key])), landing(p, dy, dx))
        if landed_early(p, dy, dx):
            n = early_pieces.index(p)
            owner = (lax.rem(ypos - dy + ny, ny) * nx + lax.rem(xpos - dx + nx, nx)) * 2 + core
            narrow(p, owner, lambda span: early[n, span])

    def gather_norm():
        lane = lax.broadcasted_iota(jnp.int32, (8, LANES), 1)
        tiles = [jnp.zeros((8, LANES), jnp.float32) for _ in range(norm_out.shape[0])]
        for s in range(n_shard):
            for c in range(n_model):
                for at in range(0, per, LANES):
                    size = min(LANES, per - at)
                    tile, shift = divmod((s * n_model + c) * per + at, LANES)
                    row = jnp.broadcast_to(norm_all[c, s, :, at:at + LANES], (8, LANES))
                    if shift:
                        row = pltpu.roll(row, shift, 1)
                    tiles[tile] = jnp.where((lane >= shift) & (lane < shift + size), row, tiles[tile])
                    if shift + size > LANES:
                        tiles[tile + 1] = jnp.where(lane < shift + size - LANES, row, tiles[tile + 1])
        for t, tile in enumerate(tiles):
            norm_rows[t:t + 1] = tile[0:1]
        norm_out[...] = norm_rows[...].astype(jnp.bfloat16)

    def norm_sum():
        wait_bytes(norm_in, norm_load)
        norm_mine[...] = jnp.zeros(norm_mine.shape, jnp.float32)
        norm_mine[:, 0:per] = norm_in[0] + norm_in[1]

    def norm_to_lead():
        @pl.when(jnp.logical_not(is_lead))
        def _():
            start(norm_mine, norm_all.at[col, me], (lead, col), mine_send, mine_recv)

    def norm_spread():
        @pl.when(is_lead)
        def _():
            norm_all[col, me] = norm_mine[...]
            wait_bytes(norm_all.at[0, pl.ds(0, n_shard - 1)], mine_recv)
            for d in range(1, n_model):
                start(norm_all.at[col], norm_all.at[col], (me, lax.rem(col + d, n_model)), z_send, z_recv)
            wait_bytes(norm_all.at[pl.ds(0, n_model - 1)], z_recv)
            gather_norm()

    def norm_out_to_chips():
        @pl.when(is_lead)
        def _():
            for d in range(1, chips):
                start(norm_out, norm_out, (lax.rem(me + 2 * d, n_shard), col), all_send, all_recv)
            start(norm_out, norm_out, (pair, col), all_send, all_recv)

    def norm_out_to_pair():
        @pl.when(jnp.logical_and(core == 1, jnp.logical_not(is_lead)))
        def _():
            wait_bytes(norm_out, all_recv)
            start(norm_out, norm_out, (pair, col), all_send, all_recv)

    average(0)

    @pl.when(is_lead)
    def _():
        pl.semaphore_wait(barrier, n_shard + n_model - 2)

    @pl.when(jnp.logical_not(is_lead))
    def _():
        pl.semaphore_wait(barrier, n_shard - 1)

    ready, chunk = 0, 0
    for n, (unit, at, width) in enumerate(spans):
        final = n == len(spans) - 1
        if final and ready > 1:
            combine_peaks(1)
        if n:
            average(n)
        if (unit, at + width) == (reach[ready][0], sum(reach[ready][1:])):
            send_peaks(ready)
            ready += 1
        if n and chunk < chunks and early_pieces:
            send_early(chunk)
            chunk += 1
    if len(groups) > 1:
        spread_peaks(1)

    for g, group in enumerate(groups):
        find_factor(g)
        before = None
        for p in [p for p in group if p not in early_pieces] + [p for p in group if p in early_pieces]:
            narrow_own(p)
            if before is not None:
                first_way(before)
            before = None if p in early_pieces else p
        if g == 0:
            norm_sum()
        if g == len(groups) - 1:
            for p in groups[0]:
                to_pair(p, 0, 0)
        if before is not None:
            first_way(before)
        if g == 0:
            for later in range(2, len(groups)):
                combine_peaks(later)
            norm_to_lead()
            for later in range(2, len(groups)):
                spread_peaks(later)
    norm_spread()
    for group in groups[1:]:
        for p in group:
            to_pair(p, 0, 0)
    norm_out_to_chips()
    for p in order:
        if p not in early_pieces:
            second_way(p)
    for p in early_pieces:
        second_way(p)

    def fill_block():
        wait_bytes(blob(paired[2]), pair_recv.at[2])
        chosen = lax.rem(ypos + 1 + core, ny) * nx + lax.rem(xpos + 2 - core, nx)
        base = 2 * rows * chosen
        width = block.shape[1]
        for c in range(2):
            @pl.when(core == c)
            def _():
                def step(i, carry):
                    block[pl.ds(pl.multiple_of(i * 16, 16), 16)] = serve_up[
                        pl.ds(pl.multiple_of(base + i * 16, 16), 16), c * width:(c + 1) * width
                    ]
                    return carry

                lax.fori_loop(0, 2 * rows // 16, step, 0, unroll=4)

    block_due = bool(near_pieces)
    for distance in range(1, ny + nx - 1):
        for own_way in (True, False):
            for p in order:
                for dy in range(ny):
                    dx = distance - dy
                    straight = (dy if along_x_first(p) else dx) == 0
                    if p in near_pieces and (dy, dx) == far:
                        continue
                    if 0 <= dx < nx and straight == own_way:
                        arrived(p, dy, dx)
                        to_x(p, dy, dx)
                        to_y(p, dy, dx)
                        to_pair(p, dy, dx)
                        if block_due and (dy, dx) == far:
                            block_due = False
                            fill_block()
            if distance == 1 and own_way:
                norm_out_to_pair()

    for unit in range(2):
        wait_bytes(blob(paired[unit]), pair_recv.at[unit])
    for kind, halves in enumerate(sent):
        if halves:
            wait_bytes(blob(halves), sent_sem.at[kind])
    for n in range(len(early_pieces)):
        wait_bytes(early.at[n, pl.ds(0, cut)], sent_sem.at[3 + n])
    wait_bytes(peaks.at[0, pl.ds(0, n_shard - 1), :, across_group(0)], peak_send.at[0])
    for g in range(1, len(groups)):
        wait_bytes(chip_peaks.at[reach[g][0], :, :, across_group(g)], peak_send.at[g])

    @pl.when(is_lead)
    def _():
        wait_bytes(norm_all.at[pl.ds(0, n_model - 1)], z_send)
        wait_bytes(blob(chips * math.prod(norm_out.shape)), all_send)

    @pl.when(jnp.logical_not(is_lead))
    def _():
        wait_bytes(norm_mine, mine_send)

    @pl.when(jnp.logical_and(core == 1, jnp.logical_not(is_lead)))
    def _():
        wait_bytes(norm_out, all_send)

    @pl.when(core == 0)
    def _():
        wait_bytes(norm_out, all_recv)


def store_kernel(count, parts, *refs):
    pairs = list(zip(refs[:count], refs[count:-1]))
    for n, (src, dst) in enumerate(pairs):
        pieces = parts if src.shape[0] % (parts * 16) == 0 else 1
        size = src.shape[0] // pieces
        for part in range(pieces):
            span = pl.ds(part * size, size)
            pltpu.make_async_copy(src.at[span], dst.at[span], refs[-1].at[n]).start()
    for n, (src, dst) in enumerate(pairs):
        pltpu.make_async_copy(src, dst, refs[-1].at[n]).wait()


def store(arrays, parts):
    hbm = pl.BlockSpec(memory_space=pltpu.HBM)
    return pl.pallas_call(
        functools.partial(store_kernel, len(arrays), parts),
        out_shape=tuple(pltpu.HBM(a.shape, a.dtype) for a in arrays),
        in_specs=[pl.BlockSpec(memory_space=pltpu.VMEM)] * len(arrays),
        out_specs=(hbm,) * len(arrays),
        scratch_shapes=[pltpu.SemaphoreType.DMA((len(arrays),))],
        compiler_params=pltpu.CompilerParams(vmem_limit_bytes=1024 * 1024),
        cost_estimate=pl.CostEstimate(flops=10**9, bytes_accessed=0, transcendentals=0),
    )(*(pltpu.with_memory_space_constraint(a, pltpu.VMEM) for a in arrays))


def patch_kernel(ny, nx, kinds, *refs):
    me = lax.axis_index("shard")
    core = lax.rem(me, 2)
    chip = me // 2
    missing = lax.rem(chip // nx + 1, ny) * nx + lax.rem(lax.rem(chip, nx) + 1, nx)
    blocks, rest, sem = refs[1:1 + len(kinds)], refs[1 + len(kinds):-1], refs[-1]
    extra, (out, *stored) = rest[:len(rest) // 2], rest[len(rest) // 2:]
    waits = []
    for n, (kind, src) in enumerate(zip(kinds, blocks)):
        height, width = src.shape
        if kind in ("direct", "swapped"):
            row = missing * height
            side = core if kind == "direct" else 1 - core
            across = pl.ds(pl.multiple_of(side * width, width), width)
        else:
            row = (2 * missing + (core if kind == "loose" else 1 - core)) * height
            across = pl.ds(out.shape[1] - width, width)
        span = pl.ds(pl.multiple_of(row, 16), height)
        waits.append(pltpu.make_async_copy(src, out.at[span, across], sem.at[n]))
        waits[-1].start()
    for n, (src, dst) in enumerate(zip(extra, stored)):
        waits.append(pltpu.make_async_copy(src, dst, sem.at[len(kinds) + n]))
        waits[-1].start()
    for copy in waits:
        copy.wait()


def patch(ny, nx, serve, blocks, extra=()):
    hbm = pl.BlockSpec(memory_space=pltpu.HBM)
    vmem = pl.BlockSpec(memory_space=pltpu.VMEM)
    held = (*blocks.values(), *extra)
    return pl.pallas_call(
        functools.partial(patch_kernel, ny, nx, tuple(blocks)),
        out_shape=tuple(pltpu.HBM(a.shape, a.dtype) for a in (serve, *extra)),
        in_specs=[hbm] + [vmem] * len(held),
        out_specs=(hbm,) * (1 + len(extra)),
        scratch_shapes=[pltpu.SemaphoreType.DMA((len(held),))],
        input_output_aliases={0: 0},
        compiler_params=pltpu.CompilerParams(vmem_limit_bytes=1024 * 1024),
        cost_estimate=pl.CostEstimate(flops=10**9, bytes_accessed=0, transcendentals=0),
    )(serve, *(pltpu.with_memory_space_constraint(a, pltpu.VMEM) for a in held))


def solution(mesh):
    n_shard, n_model = mesh.shape["shard"], mesh.shape["model"]
    ny, nx = grid_of(n_shard)
    onward_pairs, swap_pairs = [], []
    for chip in range(ny * nx):
        y, x = divmod(chip, nx)
        beside, above = y * nx + (x + 1) % nx, (y + 1) % ny * nx + x
        onward_pairs += [(2 * chip, 2 * beside), (2 * chip + 1, 2 * above + 1)]
        swap_pairs += [(2 * chip, 2 * chip + 1), (2 * chip + 1, 2 * chip)]

    def body(weight_gate, smooth_gate, weight_up, smooth_up, norm_train, norm_step):
        rows, cols = weight_gate.shape
        per = norm_train.shape[0]
        ends = min(nx, ny) > 1 and cols % (8 * LANES) == 0
        pieces = pieces_of(rows, cols, ends)
        reach = cols // LANES // 4 * LANES if ends else LANES
        spans = spans_of(pieces)
        count = len(pieces)
        wide = -(-per // LANES) * LANES
        width = n_shard * n_model * per
        tiles = -(-width // LANES)
        vmem = pl.BlockSpec(memory_space=pltpu.VMEM)
        hbm = pl.BlockSpec(memory_space=pltpu.HBM)
        dma = pltpu.SemaphoreType.DMA
        landed = pl.pallas_call(
            functools.partial(kernel, n_shard, n_model, ny, nx, pieces, spans),
            out_shape=(
                pltpu.VMEM((n_shard * rows, cols), jnp.bfloat16),
                pltpu.VMEM((n_shard * rows, cols), jnp.bfloat16),
                pltpu.VMEM((1, cols), jnp.float32),
                pltpu.VMEM((1, cols), jnp.float32),
                pltpu.VMEM((tiles, LANES), jnp.bfloat16),
                pltpu.VMEM((rows, cols), jnp.float32),
                pltpu.VMEM((rows, cols), jnp.float32),
                pltpu.VMEM((2 * rows, reach), jnp.bfloat16),
                pltpu.VMEM((rows, 2 * LANES), jnp.bfloat16),
            ),
            in_specs=[hbm] * 6,
            out_specs=(vmem,) * 9,
            scratch_shapes=[
                pltpu.VMEM((2, 2, rows, cols), jnp.float32),
                pltpu.VMEM((2, n_shard, 1, cols), jnp.float32),
                pltpu.VMEM((2, ny * nx, 1, cols), jnp.float32),
                pltpu.VMEM((2, rows, LANES), jnp.float32),
                pltpu.VMEM((2, 1, per), jnp.float32),
                pltpu.VMEM((1, wide), jnp.float32),
                pltpu.VMEM((n_model, n_shard, 1, wide), jnp.float32),
                pltpu.VMEM((tiles, LANES), jnp.float32),
                dma((len(spans),)),
                dma((3,)),
                dma((3,)),
                dma((3,)),
                dma((len(landings_of(pieces, ny, nx)),)),
                dma((3,)),
                dma((5,)),
                dma((7,)),
            ],
            compiler_params=pltpu.CompilerParams(
                collective_id=0, has_side_effects=True, vmem_limit_bytes=20 * 1024 * 1024
            ),
        )(
            *(
                pltpu.with_memory_space_constraint(a, pltpu.HBM)
                for a in (weight_gate, smooth_gate, weight_up, smooth_up, norm_train[None], norm_step[None])
            ),
        )
        *landed, whole_up, block, loose = landed
        if ends:
            direct = lax.ppermute(block, "shard", onward_pairs)
            paired = lax.ppermute(loose, "shard", swap_pairs)
        serve_gate, serve_up, factor_gate, factor_up, norm, whole_gate = store(landed, 4)
        if ends:
            direct, paired, loose, whole_up, serve_up = lax.optimization_barrier(
                (direct, paired, loose, whole_up, serve_up)
            )
            swapped = lax.ppermute(direct, "shard", swap_pairs)
            first = {"direct": direct, "loose": loose, "paired": paired}
            serve_up, whole_up = patch(ny, nx, serve_up, first, (whole_up,))
            (serve_up,) = patch(ny, nx, serve_up, {"swapped": swapped})
        else:
            (whole_up,) = store([whole_up], 4)
        return (
            serve_gate, serve_up, factor_gate.reshape(-1), factor_up.reshape(-1),
            norm.reshape(-1)[:width], whole_gate, whole_up,
        )

    in_specs = (P("shard", "model"),) * 4 + (P(("shard", "model")),) * 2
    out_specs = (
        P(None, "model"),
        P(None, "model"),
        P("model"),
        P("model"),
        P(),
        P("shard", "model"),
        P("shard", "model"),
    )
    return jax.shard_map(body, mesh=mesh, in_specs=in_specs, out_specs=out_specs, check_vma=False)
```

```python
import functools
import math

import jax
import jax.numpy as jnp
from jax import lax
from jax.experimental import pallas as pl
from jax.experimental.pallas import tpu as pltpu
from jax.sharding import PartitionSpec as P

MESH = pl.DeviceIdType.MESH
keep_rate = 0.7
LANES = 128


def grid_of(n_shard):
    chips = n_shard // 2
    nx = math.isqrt(chips)
    while chips % nx:
        nx -= 1
    return chips // nx, nx


def pieces_of(rows, cols, ends):
    tiles = cols // LANES
    cut = rows * 3 // 4 // 16 * 16
    found, tails = [], []
    for unit in range(2):
        at = 0
        queues = []
        for along_x, many in ((True, (tiles + 1) // 2), (False, tiles // 2)):
            if many < 4 or not ends:
                queues.append([(along_x, 1, None)] * many)
            elif unit == 0:
                queues.append([(along_x, 2, None), (along_x, 1, "early"), (along_x, many - 3, None)])
            else:
                near = many // 2
                queues.append([(along_x, near, "near"), (along_x, many - near - 1, None), (along_x, 1, "loose")])
        for n in range(max(len(q) for q in queues)):
            for queue in queues:
                if n < len(queue):
                    along_x, width, kind = queue[n]
                    here = (unit, at * LANES, width * LANES)
                    at += width
                    if kind == "early":
                        found.append(here + (0, cut, along_x, kind))
                        tails.append(here + (cut, rows - cut, along_x, None))
                    else:
                        found.append(here + (0, rows, along_x, kind))
        found += tails
        tails = []
    return found


def is_early_landing(piece, dy, dx):
    return piece[6] == "early" and (dy, dx) == ((0, 1) if piece[5] else (1, 0))


def landings_of(pieces, ny, nx):
    found = {}
    far = (ny - 1, nx - 1)
    for p, piece in enumerate(pieces):
        unit, along_x, kind = piece[0], piece[5], piece[6]
        for dy in range(ny):
            for dx in range(nx):
                if (dy, dx) == (0, 0) or (kind == "near" and (dy, dx) == far):
                    continue
                key = (unit, along_x, dy, dx)
                if (dy, dx) == ((1, 0) if along_x else (0, 1)):
                    key = unit
                elif is_early_landing(piece, dy, dx) or (unit and (dy, dx) == far):
                    key = (p, dy, dx)
                found.setdefault(key, []).append((p, dy, dx))
    return found


def spans_of(pieces):
    spans = []
    for unit, at, width, top, _, _, _ in pieces:
        if top:
            continue
        if spans and spans[-1][0] == unit and spans[-1][2] == width and width <= 2 * LANES:
            spans[-1] = (unit, spans[-1][1], spans[-1][2] + width)
        else:
            spans.append((unit, at, width))
    return spans


def kernel(
    n_shard, n_model, ny, nx, pieces, spans,
    weight_gate, smooth_gate, weight_up, smooth_up, norm_train, norm_step,
    serve_gate, serve_up, factor_gate, factor_up, norm_out, whole_gate, whole_up, block, loose,
    inputs, peaks, chip_peaks, early, norm_in, norm_mine, norm_all, norm_rows,
    load_sem, peak_send, peak_recv, couple_recv, ring_recv, pair_recv, sent_sem, small_sem,
):
    me = lax.axis_index("shard")
    col = lax.axis_index("model")
    core = lax.rem(me, 2)
    chip = me // 2
    xpos, ypos = lax.rem(chip, nx), chip // nx
    x_next = (ypos * nx + lax.rem(xpos + 1, nx)) * 2 + core
    y_next = (lax.rem(ypos + 1, ny) * nx + xpos) * 2 + core
    pair = chip * 2 + (1 - core)
    rows, cols = whole_gate.shape
    serves, wholes, factors = (serve_gate, serve_up), (whole_gate, whole_up), (factor_gate, factor_up)
    order = range(len(pieces))
    early_pieces = [p for p in order if pieces[p][6] == "early"]
    loose_pieces = [p for p in order if pieces[p][6] == "loose"]
    near_pieces = [p for p in order if pieces[p][6] == "near"]
    far = (ny - 1, nx - 1)
    chips = ny * nx
    lead = 1
    is_lead = me == lead
    per = norm_train.shape[1]
    norm_load, mine_send, mine_recv, z_send, z_recv, all_send, all_recv = [small_sem.at[i] for i in range(7)]

    def across(p):
        return pl.ds(pieces[p][1], pieces[p][2])

    def wait_bytes(ref, sem):
        pltpu.make_async_copy(ref, ref, sem).wait()

    def blob(halves):
        wide = next(
            w for w in range(LANES, cols + 1, LANES) if halves % (8 * w) == 0 and halves // w <= n_shard * rows
        )
        return serve_gate.at[pl.ds(0, halves // wide), pl.ds(0, wide)]

    groups = [[], [], []]
    for p in order:
        unit, at = pieces[p][:2]
        groups[2 if unit else int(at >= sum(spans[0][1:]))].append(p)
    groups = [g for g in groups if g]
    reach = [
        (pieces[g[0]][0], pieces[g[0]][1], sum(pieces[p][2] for p in g if pieces[p][3] == 0)) for g in groups
    ]

    barrier = pltpu.get_barrier_semaphore()
    for d in range(1, n_shard):
        pl.semaphore_signal(barrier, inc=1, device_id=(lax.rem(me + d, n_shard), col), device_id_type=MESH)

    @pl.when(is_lead)
    def _():
        for d in range(1, n_model):
            pl.semaphore_signal(barrier, inc=1, device_id=(me, lax.rem(col + d, n_model)), device_id_type=MESH)

    sources = ((weight_gate, smooth_gate), (weight_up, smooth_up))
    for n, (unit, at, width) in enumerate(spans):
        for which in range(2):
            pltpu.make_async_copy(
                sources[unit][which].at[:, pl.ds(at, width)], inputs.at[which, unit, :, pl.ds(at, width)], load_sem.at[n]
            ).start()
    for i, src in enumerate((norm_train, norm_step)):
        pltpu.make_async_copy(src, norm_in.at[i], norm_load).start()

    def average(n):
        unit, first, width = spans[n]
        here = pl.ds(first, width)
        wait_bytes(inputs.at[:, unit, :, here], load_sem.at[n])

        def step(i, top):
            rows_now = pl.ds(pl.multiple_of(i * 8, 8), 8)
            value = keep_rate * inputs[1, unit, rows_now, here] + (1.0 - keep_rate) * inputs[0, unit, rows_now, here]
            wholes[unit][rows_now, here] = value
            return jnp.maximum(top, jnp.abs(value))

        top = lax.fori_loop(0, rows // 8, step, jnp.zeros((8, width), jnp.float32), unroll=4)
        peaks[unit, me, :, here] = jnp.max(top, axis=0, keepdims=True)

    def start(src, dst, device, send_sem, recv_sem):
        pltpu.make_async_remote_copy(
            src_ref=src, dst_ref=dst, send_sem=send_sem, recv_sem=recv_sem,
            device_id=device, device_id_type=MESH,
        ).start()

    def across_group(g):
        return pl.ds(reach[g][1], reach[g][2])

    def send_peaks(g):
        ref = peaks.at[reach[g][0], me, :, across_group(g)]
        if g == 0:
            for d in range(1, n_shard):
                start(ref, ref, (lax.rem(me + d, n_shard), col), peak_send.at[g], peak_recv.at[g])
        else:
            start(ref, ref, (pair, col), peak_send.at[g], couple_recv.at[g])

    def combine_peaks(g):
        unit, here = reach[g][0], across_group(g)
        wait_bytes(peaks.at[unit, 0, :, here], couple_recv.at[g])
        chip_peaks[unit, chip, :, here] = jnp.maximum(peaks[unit, me, :, here], peaks[unit, pair, :, here])

    def spread_peaks(g):
        ref = chip_peaks.at[reach[g][0], chip, :, across_group(g)]
        for d in range(1, chips):
            start(ref, ref, (lax.rem(me + 2 * d, n_shard), col), peak_send.at[g], peak_recv.at[g])

    def piece_of(p, dy, dx, side):
        owner = (lax.rem(ypos - dy + ny, ny) * nx + lax.rem(xpos - dx + nx, nx)) * 2 + side
        unit, _, _, top, height = pieces[p][:5]
        return serves[unit].at[pl.ds(pl.multiple_of(owner * rows + top, 16), height), across(p)]

    def along_x_first(p):
        return pieces[p][5]

    def landed_early(p, dy, dx):
        return is_early_landing(pieces[p], dy, dx)

    gathers = landings_of(pieces, ny, nx)
    keys = list(gathers)

    def key_of(p, dy, dx):
        return next(key for key in keys if (p, dy, dx) in gathers[key])

    def landing(p, dy, dx):
        return ring_recv.at[keys.index(key_of(p, dy, dx))]

    sent = [0, 0, 0]
    paired = [0, 0, 0]

    def send(p, spot, device, sem, dst=None):
        ref = piece_of(p, *spot, core)
        kind = 2 if p in early_pieces else pieces[p][0]
        sent[kind] += pieces[p][2] * pieces[p][4]
        start(ref, ref if dst is None else dst, (device, col), sent_sem.at[kind], sem)

    def loose_ref(p):
        return loose.at[:, pl.ds(loose_pieces.index(p) * LANES, LANES)]

    def onward(p, spot, device, there):
        if p in near_pieces and there == far:
            return
        send(p, spot, device, landing(p, *there), loose_ref(p) if p in loose_pieces and there == far else None)

    def to_x(p, dy, dx):
        if dx < nx - 1 and (dy == 0 or not along_x_first(p)):
            onward(p, (dy, dx), x_next, (dy, dx + 1))

    def to_y(p, dy, dx):
        if dy < ny - 1 and (dx == 0 or along_x_first(p)):
            onward(p, (dy, dx), y_next, (dy + 1, dx))

    def to_pair(p, dy, dx):
        if not (p in loose_pieces and (dy, dx) == far):
            kind = 2 if p in near_pieces else pieces[p][0]
            paired[kind] += pieces[p][2] * pieces[p][4]
            send(p, (dy, dx), pair, pair_recv.at[kind])

    def first_way(p):
        (to_x if along_x_first(p) else to_y)(p, 0, 0)

    def second_way(p):
        (to_y if along_x_first(p) else to_x)(p, 0, 0)

    cut = pieces[early_pieces[0]][4] if early_pieces else 0
    chunks = 3 if cut % 24 == 0 else 1

    def send_early(chunk):
        span = pl.ds(chunk * (cut // chunks), cut // chunks)
        for n, p in enumerate(early_pieces):
            device, spot = (x_next, (0, 1)) if along_x_first(p) else (y_next, (1, 0))
            start(
                wholes[pieces[p][0]].at[span, across(p)], early.at[n, span], (device, col),
                sent_sem.at[3 + n], landing(p, *spot),
            )

    def find_factor(g):
        unit, here = reach[g][0], across_group(g)
        table, many = (peaks, n_shard) if g == 0 else (chip_peaks, chips)
        if many > 1:
            wait_bytes(table.at[unit, pl.ds(0, many - 1), :, here], peak_recv.at[g])
        factor = table[unit, 0, :, here]
        for d in range(1, many):
            factor = jnp.maximum(factor, table[unit, d, :, here])
        factors[unit][:, here] = factor

    def narrow(p, owner, read):
        unit, _, _, top, height = pieces[p][:5]

        def step(i, carry):
            at = top + i * 16
            value = read(pl.ds(pl.multiple_of(at, 16), 16)) / factors[unit][:, across(p)]
            serves[unit][pl.ds(pl.multiple_of(owner * rows + at, 16), 16), across(p)] = value.astype(jnp.bfloat16)
            return carry

        lax.fori_loop(0, height // 16, step, 0, unroll=2)

    def narrow_own(p):
        narrow(p, me, lambda span: wholes[pieces[p][0]][span, across(p)])

    here_now = set()

    def arrived(p, dy, dx):
        key = key_of(p, dy, dx)
        if key not in here_now:
            here_now.add(key)
            if landed_early(p, dy, dx):
                wait_bytes(early.at[early_pieces.index(p), pl.ds(0, cut)], landing(p, dy, dx))
            else:
                wait_bytes(blob(sum(pieces[q][2] * pieces[q][4] for q, _, _ in gathers[key])), landing(p, dy, dx))
        if landed_early(p, dy, dx):
            n = early_pieces.index(p)
            owner = (lax.rem(ypos - dy + ny, ny) * nx + lax.rem(xpos - dx + nx, nx)) * 2 + core
            narrow(p, owner, lambda span: early[n, span])

    def gather_norm():
        lane = lax.broadcasted_iota(jnp.int32, (8, LANES), 1)
        tiles = [jnp.zeros((8, LANES), jnp.float32) for _ in range(norm_out.shape[0])]
        for s in range(n_shard):
            for c in range(n_model):
                for at in range(0, per, LANES):
                    size = min(LANES, per - at)
                    tile, shift = divmod((s * n_model + c) * per + at, LANES)
                    row = jnp.broadcast_to(norm_all[c, s, :, at:at + LANES], (8, LANES))
                    if shift:
                        row = pltpu.roll(row, shift, 1)
                    tiles[tile] = jnp.where((lane >= shift) & (lane < shift + size), row, tiles[tile])
                    if shift + size > LANES:
                        tiles[tile + 1] = jnp.where(lane < shift + size - LANES, row, tiles[tile + 1])
        for t, tile in enumerate(tiles):
            norm_rows[t:t + 1] = tile[0:1]
        norm_out[...] = norm_rows[...].astype(jnp.bfloat16)

    def norm_sum():
        wait_bytes(norm_in, norm_load)
        norm_mine[...] = jnp.zeros(norm_mine.shape, jnp.float32)
        norm_mine[:, 0:per] = norm_in[0] + norm_in[1]

    def norm_to_lead():
        @pl.when(jnp.logical_not(is_lead))
        def _():
            start(norm_mine, norm_all.at[col, me], (lead, col), mine_send, mine_recv)

    def norm_spread():
        @pl.when(is_lead)
        def _():
            norm_all[col, me] = norm_mine[...]
            wait_bytes(norm_all.at[0, pl.ds(0, n_shard - 1)], mine_recv)
            for d in range(1, n_model):
                start(norm_all.at[col], norm_all.at[col], (me, lax.rem(col + d, n_model)), z_send, z_recv)
            wait_bytes(norm_all.at[pl.ds(0, n_model - 1)], z_recv)
            gather_norm()

    def norm_out_to_chips():
        @pl.when(is_lead)
        def _():
            for d in range(1, chips):
                start(norm_out, norm_out, (lax.rem(me + 2 * d, n_shard), col), all_send, all_recv)
            start(norm_out, norm_out, (pair, col), all_send, all_recv)

    def norm_out_to_pair():
        @pl.when(jnp.logical_and(core == 1, jnp.logical_not(is_lead)))
        def _():
            wait_bytes(norm_out, all_recv)
            start(norm_out, norm_out, (pair, col), all_send, all_recv)

    average(0)

    @pl.when(is_lead)
    def _():
        pl.semaphore_wait(barrier, n_shard + n_model - 2)

    @pl.when(jnp.logical_not(is_lead))
    def _():
        pl.semaphore_wait(barrier, n_shard - 1)

    ready, chunk = 0, 0
    for n, (unit, at, width) in enumerate(spans):
        final = n == len(spans) - 1
        if final and ready > 1:
            combine_peaks(1)
        if n:
            average(n)
        if (unit, at + width) == (reach[ready][0], sum(reach[ready][1:])):
            send_peaks(ready)
            ready += 1
        if n and chunk < chunks and early_pieces:
            send_early(chunk)
            chunk += 1
    if len(groups) > 1:
        spread_peaks(1)

    for g, group in enumerate(groups):
        find_factor(g)
        before = None
        for p in [p for p in group if p not in early_pieces] + [p for p in group if p in early_pieces]:
            narrow_own(p)
            if before is not None:
                first_way(before)
            before = None if p in early_pieces else p
        if g == 0:
            norm_sum()
        if g == len(groups) - 1:
            for p in groups[0]:
                to_pair(p, 0, 0)
        if before is not None:
            first_way(before)
        if g == 0:
            for later in range(2, len(groups)):
                combine_peaks(later)
            norm_to_lead()
            for later in range(2, len(groups)):
                spread_peaks(later)
    norm_spread()
    for group in groups[1:]:
        for p in group:
            to_pair(p, 0, 0)
    norm_out_to_chips()
    for p in order:
        if p not in early_pieces:
            second_way(p)
    for p in early_pieces:
        second_way(p)

    def fill_block():
        wait_bytes(blob(paired[2]), pair_recv.at[2])
        chosen = lax.rem(ypos + 1 + core, ny) * nx + lax.rem(xpos + 2 - core, nx)
        base = 2 * rows * chosen
        width = block.shape[1]
        for c in range(2):
            @pl.when(core == c)
            def _():
                def step(i, carry):
                    block[pl.ds(pl.multiple_of(i * 16, 16), 16)] = serve_up[
                        pl.ds(pl.multiple_of(base + i * 16, 16), 16), c * width:(c + 1) * width
                    ]
                    return carry

                lax.fori_loop(0, 2 * rows // 16, step, 0, unroll=4)

    block_due = bool(near_pieces)
    for distance in range(1, ny + nx - 1):
        for own_way in (True, False):
            for p in order:
                for dy in range(ny):
                    dx = distance - dy
                    straight = (dy if along_x_first(p) else dx) == 0
                    if p in near_pieces and (dy, dx) == far:
                        continue
                    if 0 <= dx < nx and straight == own_way:
                        arrived(p, dy, dx)
                        to_x(p, dy, dx)
                        to_y(p, dy, dx)
                        to_pair(p, dy, dx)
                        if block_due and (dy, dx) == far:
                            block_due = False
                            fill_block()
            if distance == 1 and own_way:
                norm_out_to_pair()

    for unit in range(2):
        wait_bytes(blob(paired[unit]), pair_recv.at[unit])
    for kind, halves in enumerate(sent):
        if halves:
            wait_bytes(blob(halves), sent_sem.at[kind])
    for n in range(len(early_pieces)):
        wait_bytes(early.at[n, pl.ds(0, cut)], sent_sem.at[3 + n])
    wait_bytes(peaks.at[0, pl.ds(0, n_shard - 1), :, across_group(0)], peak_send.at[0])
    for g in range(1, len(groups)):
        wait_bytes(chip_peaks.at[reach[g][0], :, :, across_group(g)], peak_send.at[g])

    @pl.when(is_lead)
    def _():
        wait_bytes(norm_all.at[pl.ds(0, n_model - 1)], z_send)
        wait_bytes(blob(chips * math.prod(norm_out.shape)), all_send)

    @pl.when(jnp.logical_not(is_lead))
    def _():
        wait_bytes(norm_mine, mine_send)

    @pl.when(jnp.logical_and(core == 1, jnp.logical_not(is_lead)))
    def _():
        wait_bytes(norm_out, all_send)

    @pl.when(core == 0)
    def _():
        wait_bytes(norm_out, all_recv)


def store_kernel(count, parts, *refs):
    pairs = list(zip(refs[:count], refs[count:-1]))
    for n, (src, dst) in enumerate(pairs):
        pieces = parts if src.shape[0] % (parts * 16) == 0 else 1
        size = src.shape[0] // pieces
        for part in range(pieces):
            span = pl.ds(part * size, size)
            pltpu.make_async_copy(src.at[span], dst.at[span], refs[-1].at[n]).start(priority=(part + n) % 2)
    for n, (src, dst) in enumerate(pairs):
        pltpu.make_async_copy(src, dst, refs[-1].at[n]).wait()


def store(arrays, parts):
    hbm = pl.BlockSpec(memory_space=pltpu.HBM)
    return pl.pallas_call(
        functools.partial(store_kernel, len(arrays), parts),
        out_shape=tuple(pltpu.HBM(a.shape, a.dtype) for a in arrays),
        in_specs=[pl.BlockSpec(memory_space=pltpu.VMEM)] * len(arrays),
        out_specs=(hbm,) * len(arrays),
        scratch_shapes=[pltpu.SemaphoreType.DMA((len(arrays),))],
        compiler_params=pltpu.CompilerParams(vmem_limit_bytes=1024 * 1024),
        cost_estimate=pl.CostEstimate(flops=10**9, bytes_accessed=0, transcendentals=0),
    )(*(pltpu.with_memory_space_constraint(a, pltpu.VMEM) for a in arrays))


def patch_kernel(ny, nx, kinds, *refs):
    me = lax.axis_index("shard")
    core = lax.rem(me, 2)
    chip = me // 2
    missing = lax.rem(chip // nx + 1, ny) * nx + lax.rem(lax.rem(chip, nx) + 1, nx)
    blocks, rest, sem = refs[1:1 + len(kinds)], refs[1 + len(kinds):-1], refs[-1]
    extra, (out, *stored) = rest[:len(rest) // 2], rest[len(rest) // 2:]
    waits = []
    for n, (kind, src) in enumerate(zip(kinds, blocks)):
        height, width = src.shape
        if kind in ("direct", "swapped"):
            row = missing * height
            side = core if kind == "direct" else 1 - core
            across = pl.ds(pl.multiple_of(side * width, width), width)
        else:
            row = (2 * missing + (core if kind == "loose" else 1 - core)) * height
            across = pl.ds(out.shape[1] - width, width)
        span = pl.ds(pl.multiple_of(row, 16), height)
        waits.append(pltpu.make_async_copy(src, out.at[span, across], sem.at[n]))
        waits[-1].start()
    for n, (src, dst) in enumerate(zip(extra, stored)):
        waits.append(pltpu.make_async_copy(src, dst, sem.at[len(kinds) + n]))
        waits[-1].start()
    for copy in waits:
        copy.wait()


def patch(ny, nx, serve, blocks, extra=()):
    hbm = pl.BlockSpec(memory_space=pltpu.HBM)
    vmem = pl.BlockSpec(memory_space=pltpu.VMEM)
    held = (*blocks.values(), *extra)
    return pl.pallas_call(
        functools.partial(patch_kernel, ny, nx, tuple(blocks)),
        out_shape=tuple(pltpu.HBM(a.shape, a.dtype) for a in (serve, *extra)),
        in_specs=[hbm] + [vmem] * len(held),
        out_specs=(hbm,) * (1 + len(extra)),
        scratch_shapes=[pltpu.SemaphoreType.DMA((len(held),))],
        input_output_aliases={0: 0},
        compiler_params=pltpu.CompilerParams(vmem_limit_bytes=1024 * 1024),
        cost_estimate=pl.CostEstimate(flops=10**9, bytes_accessed=0, transcendentals=0),
    )(serve, *(pltpu.with_memory_space_constraint(a, pltpu.VMEM) for a in held))


def solution(mesh):
    n_shard, n_model = mesh.shape["shard"], mesh.shape["model"]
    ny, nx = grid_of(n_shard)
    onward_pairs, swap_pairs = [], []
    for chip in range(ny * nx):
        y, x = divmod(chip, nx)
        beside, above = y * nx + (x + 1) % nx, (y + 1) % ny * nx + x
        onward_pairs += [(2 * chip, 2 * beside), (2 * chip + 1, 2 * above + 1)]
        swap_pairs += [(2 * chip, 2 * chip + 1), (2 * chip + 1, 2 * chip)]

    def body(weight_gate, smooth_gate, weight_up, smooth_up, norm_train, norm_step):
        rows, cols = weight_gate.shape
        per = norm_train.shape[0]
        ends = min(nx, ny) > 1 and cols % (8 * LANES) == 0
        pieces = pieces_of(rows, cols, ends)
        reach = cols // LANES // 4 * LANES if ends else LANES
        spans = spans_of(pieces)
        count = len(pieces)
        wide = -(-per // LANES) * LANES
        width = n_shard * n_model * per
        tiles = -(-width // LANES)
        vmem = pl.BlockSpec(memory_space=pltpu.VMEM)
        hbm = pl.BlockSpec(memory_space=pltpu.HBM)
        dma = pltpu.SemaphoreType.DMA
        landed = pl.pallas_call(
            functools.partial(kernel, n_shard, n_model, ny, nx, pieces, spans),
            out_shape=(
                pltpu.VMEM((n_shard * rows, cols), jnp.bfloat16),
                pltpu.VMEM((n_shard * rows, cols), jnp.bfloat16),
                pltpu.VMEM((1, cols), jnp.float32),
                pltpu.VMEM((1, cols), jnp.float32),
                pltpu.VMEM((tiles, LANES), jnp.bfloat16),
                pltpu.VMEM((rows, cols), jnp.float32),
                pltpu.VMEM((rows, cols), jnp.float32),
                pltpu.VMEM((2 * rows, reach), jnp.bfloat16),
                pltpu.VMEM((rows, 2 * LANES), jnp.bfloat16),
            ),
            in_specs=[hbm] * 6,
            out_specs=(vmem,) * 9,
            scratch_shapes=[
                pltpu.VMEM((2, 2, rows, cols), jnp.float32),
                pltpu.VMEM((2, n_shard, 1, cols), jnp.float32),
                pltpu.VMEM((2, ny * nx, 1, cols), jnp.float32),
                pltpu.VMEM((2, rows, LANES), jnp.float32),
                pltpu.VMEM((2, 1, per), jnp.float32),
                pltpu.VMEM((1, wide), jnp.float32),
                pltpu.VMEM((n_model, n_shard, 1, wide), jnp.float32),
                pltpu.VMEM((tiles, LANES), jnp.float32),
                dma((len(spans),)),
                dma((3,)),
                dma((3,)),
                dma((3,)),
                dma((len(landings_of(pieces, ny, nx)),)),
                dma((3,)),
                dma((5,)),
                dma((7,)),
            ],
            compiler_params=pltpu.CompilerParams(
                collective_id=0, has_side_effects=True, vmem_limit_bytes=20 * 1024 * 1024
            ),
        )(
            *(
                pltpu.with_memory_space_constraint(a, pltpu.HBM)
                for a in (weight_gate, smooth_gate, weight_up, smooth_up, norm_train[None], norm_step[None])
            ),
        )
        *landed, whole_up, block, loose = landed
        if ends:
            direct = lax.ppermute(block, "shard", onward_pairs)
            paired = lax.ppermute(loose, "shard", swap_pairs)
        serve_gate, serve_up, factor_gate, factor_up, norm, whole_gate = store(landed, 8)
        if ends:
            direct, paired, loose, whole_up, serve_up = lax.optimization_barrier(
                (direct, paired, loose, whole_up, serve_up)
            )
            swapped = lax.ppermute(direct, "shard", swap_pairs)
            first = {"direct": direct, "loose": loose, "paired": paired}
            serve_up, whole_up = patch(ny, nx, serve_up, first, (whole_up,))
            (serve_up,) = patch(ny, nx, serve_up, {"swapped": swapped})
        else:
            (whole_up,) = store([whole_up], 4)
        return (
            serve_gate, serve_up, factor_gate.reshape(-1), factor_up.reshape(-1),
            norm.reshape(-1)[:width], whole_gate, whole_up,
        )

    in_specs = (P("shard", "model"),) * 4 + (P(("shard", "model")),) * 2
    out_specs = (
        P(None, "model"),
        P(None, "model"),
        P("model"),
        P("model"),
        P(),
        P("shard", "model"),
        P("shard", "model"),
    )
    return jax.shard_map(body, mesh=mesh, in_specs=in_specs, out_specs=out_specs, check_vma=False)
```
